16 devices in a mesh: dp: 2 (over z), tp: 8 (over y, x, core).
Axes of the slice: x: 2, y: 2, z: 2, core: 2. Of those that a mesh axis runs over, the one named last changes fastest.
Arguments:
- token_ids: int32 [4, 256], P('dp'), parts along dimension 0
- emb_table: bfloat16 [512, 4096], P('tp')
- gain_vec: bfloat16 [4096], replicated
- w_qkv: bfloat16 [4096, 34816], P(None, 'tp')
- grad_u: bfloat16 [4, 256, 34816], P('dp', None, 'tp'), parts along dimension 0
- grad_res: bfloat16 [4, 256, 4096], P('dp', 'tp'), parts along dimension 0
Outputs:
- output 1: bfloat16 [4, 256, 34816], P('dp', None, 'tp'), parts along dimension 0
- output 2: bfloat16 [4, 256, 4096], P('dp', 'tp'), parts along dimension 0
- output 3: float32 [1024, 4096], P(('dp', 'tp')), parts along dimension 0
- output 4: float32 [4096, 69632], P(None, ('dp', 'tp')), parts along dimension 1
- output 5: float32 [8192], P('dp'), parts along dimension 0
There are 2 independent parts. The reference program is written for one: setup_inputs(seed, part) draws one part's arguments, and reference() takes and returns one part's arrays. A program takes and returns all parts, laid end to end along the dimension named above; an argument that names none is the same for every part.
All inputs are finite; a program needn't handle non-finite values.
Results may differ from the reference program's by a relative error of at most 0.00497172.
Values are sent between devices in bfloat16 or wider.
A program may use at most 1 GiB of HBM per device.

```python
import jax
import jax.numpy as jnp
from jax import lax

NUM_MICRO = 2
SEQ_LEN = 256
VOCAB_ROWS = 512
MODEL_DIM = 4096
QKV_COLS = 34816
GROUP_SIZE = 8
COLS_DEV = QKV_COLS // GROUP_SIZE
NORM_EPS = 1e-6


def setup_inputs(seed: int = 0, part: int = 0) -> dict:
    root_key = jax.random.key(seed)
    own_keys = jax.random.split(jax.random.fold_in(root_key, part), 6)
    shared_keys = jax.random.split(root_key, 3)
    spacing = VOCAB_ROWS // 64
    base_ids = jax.random.randint(own_keys[0], (NUM_MICRO, SEQ_LEN), 0, VOCAB_ROWS)
    hot_slot = jax.random.randint(own_keys[1], (NUM_MICRO, SEQ_LEN), 0, 64)
    hot_shift = jax.random.randint(own_keys[2], (), 0, spacing)
    use_hot = jax.random.randint(own_keys[3], (NUM_MICRO, SEQ_LEN), 0, 2)
    token_ids = jnp.where(use_hot == 1, hot_slot * spacing + hot_shift, base_ids)
    token_ids = token_ids.at[0, 0].set(0).at[0, 1].set(VOCAB_ROWS - 1).astype(jnp.int32)
    emb_table = jax.random.normal(shared_keys[0], (VOCAB_ROWS, MODEL_DIM), jnp.float32).astype(jnp.bfloat16)
    gain_vec = (0.5 + jax.random.uniform(shared_keys[1], (MODEL_DIM,), jnp.float32)).astype(jnp.bfloat16)
    w_qkv = (jax.random.normal(shared_keys[2], (MODEL_DIM, QKV_COLS), jnp.float32) * MODEL_DIM ** -0.5).astype(jnp.bfloat16)
    grad_u = (jax.random.normal(own_keys[4], (NUM_MICRO, SEQ_LEN, QKV_COLS), jnp.float32) * (MODEL_DIM / QKV_COLS) ** 0.5).astype(jnp.bfloat16)
    grad_res = jax.random.normal(own_keys[5], (NUM_MICRO, SEQ_LEN, MODEL_DIM), jnp.float32).astype(jnp.bfloat16)
    return {'token_ids': token_ids, 'emb_table': emb_table, 'gain_vec': gain_vec, 'w_qkv': w_qkv, 'grad_u': grad_u, 'grad_res': grad_res}


def reference(token_ids, emb_table, gain_vec, w_qkv, grad_u, grad_res):
    gain_f = gain_vec.astype(jnp.float32)

    def micro_step(acc_state, inputs):
        grad_table, grad_w, grad_gain = acc_state
        tok_ids, du_m, dres_m = inputs
        tokens = jnp.take(emb_table, tok_ids, axis=0)
        tok_f = tokens.astype(jnp.float32)
        inv_rms = lax.rsqrt(jnp.mean(tok_f * tok_f, axis=-1, keepdims=True) + NORM_EPS)
        n_hat = tok_f * inv_rms
        normed = (n_hat * gain_f).astype(jnp.bfloat16)
        u_m = jnp.dot(normed, w_qkv, preferred_element_type=jnp.float32).astype(jnp.bfloat16)

        def group_term(dn_acc, group_idx):
            du_r = lax.dynamic_slice_in_dim(du_m, group_idx * COLS_DEV, COLS_DEV, axis=1)
            w_r = lax.dynamic_slice_in_dim(w_qkv, group_idx * COLS_DEV, COLS_DEV, axis=1)
            part_dn = jnp.dot(du_r, w_r.T, preferred_element_type=jnp.float32).astype(jnp.bfloat16)
            return dn_acc + part_dn.astype(jnp.float32), None

        d_norm, _ = lax.scan(group_term, jnp.zeros((SEQ_LEN, MODEL_DIM), jnp.float32), jnp.arange(GROUP_SIZE))
        gain_dn = gain_f * d_norm
        centre = jnp.mean(n_hat * gain_dn, axis=-1, keepdims=True)
        d_x = (dres_m.astype(jnp.float32) + inv_rms * (gain_dn - n_hat * centre)).astype(jnp.bfloat16)
        grad_table = grad_table + jax.ops.segment_sum(d_x.astype(jnp.float32), tok_ids, num_segments=VOCAB_ROWS)
        grad_w = grad_w + jnp.dot(normed.T, du_m, preferred_element_type=jnp.float32)
        grad_gain = grad_gain + jnp.sum(d_norm * n_hat, axis=0)
        return (grad_table, grad_w, grad_gain), (u_m, tokens)

    init_state = (jnp.zeros((VOCAB_ROWS, MODEL_DIM), jnp.float32), jnp.zeros((MODEL_DIM, QKV_COLS), jnp.float32), jnp.zeros((MODEL_DIM,), jnp.float32))
    (grad_table, grad_w, grad_gain), (u_proj, x_resid) = lax.scan(micro_step, init_state, (token_ids, grad_u, grad_res))
    return u_proj, x_resid, grad_table, grad_w, grad_gain
```

```python
import jax
import jax.numpy as jnp
from jax import lax
from jax.sharding import PartitionSpec as P

NORM_EPS = 1e-6


def solution(mesh):
    group_size = mesh.shape['tp']

    def local_step(token_ids, table_loc, gain_vec, w_loc, du_loc, dres_loc):
        num_micro, seq_len = token_ids.shape
        rows_loc, model_dim = table_loc.shape
        seq_loc = seq_len // group_size
        cols_loc = w_loc.shape[1]
        tokens_all = num_micro * seq_len
        dev_idx = lax.axis_index('tp')
        gain_f = gain_vec.astype(jnp.float32)
        du_flat = du_loc.reshape(tokens_all, cols_loc)

        dn_part = lax.dot_general(du_flat, w_loc, (((1,), (1,)), ((), ())), preferred_element_type=jnp.float32).astype(jnp.bfloat16)
        dn_part = dn_part.reshape(num_micro, group_size, seq_loc, model_dim).transpose(1, 0, 2, 3)
        dn_recv = lax.all_to_all(dn_part, 'tp', 0, 0, tiled=True)
        d_norm = jnp.sum(dn_recv, axis=0, dtype=jnp.float32)

        table = lax.all_gather(table_loc, 'tp', axis=0, tiled=True)
        tab_f = table.astype(jnp.float32)
        inv_tab = lax.rsqrt(jnp.mean(tab_f * tab_f, axis=-1, keepdims=True) + NORM_EPS)
        n_tab = (tab_f * inv_tab * gain_f).astype(jnp.bfloat16)
        ids_flat = token_ids.reshape(tokens_all)
        normed = jnp.take(n_tab, ids_flat, axis=0)
        u_all = jnp.dot(normed, w_loc, preferred_element_type=jnp.float32).astype(jnp.bfloat16)
        grad_w = lax.dot_general(normed, du_flat, (((0,), (0,)), ((), ())), preferred_element_type=jnp.float32)

        own_ids = lax.dynamic_slice_in_dim(token_ids, dev_idx * seq_loc, seq_loc, axis=1)
        x_own = jnp.take(table, own_ids, axis=0)
        x_f = x_own.astype(jnp.float32)
        inv_own = lax.rsqrt(jnp.mean(x_f * x_f, axis=-1, keepdims=True) + NORM_EPS)
        hat_own = x_f * inv_own
        gain_dn = gain_f * d_norm
        centre = jnp.mean(hat_own * gain_dn, axis=-1, keepdims=True)
        d_x = (dres_loc.astype(jnp.float32) + inv_own * (gain_dn - hat_own * centre)).astype(jnp.bfloat16)
        grad_gain = lax.psum(jnp.sum(d_norm * hat_own, axis=(0, 1)), 'tp')
        dx_all = lax.all_gather(d_x, 'tp', axis=1, tiled=True).reshape(tokens_all, model_dim)
        pick = (ids_flat[None, :] == dev_idx * rows_loc + lax.broadcasted_iota(jnp.int32, (rows_loc, tokens_all), 0)).astype(jnp.bfloat16)
        grad_table = jnp.dot(pick, dx_all, preferred_element_type=jnp.float32)
        return u_all.reshape(num_micro, seq_len, cols_loc), x_own, grad_table, grad_w, grad_gain

    return jax.shard_map(local_step, mesh=mesh,
                         in_specs=(P('dp', None), P('tp', None), P(None), P(None, 'tp'), P('dp', None, 'tp'), P('dp', 'tp', None)),
                         out_specs=(P('dp', None, 'tp'), P('dp', 'tp', None), P(('dp', 'tp'), None), P(None, ('dp', 'tp')), P('dp')),
                         check_vma=False)
```

```python
import functools

import jax
import jax.numpy as jnp
from jax import lax
from jax.experimental import pallas as pl
from jax.experimental.pallas import tpu as pltpu
from jax.sharding import PartitionSpec as P

NORM_EPS = 1e-6
MESH = pl.DeviceIdType.MESH
F32 = jnp.float32
BF16 = jnp.bfloat16
FB = 512
NB = 8
UC = 256
TB = 128


def _flip(r, bits):
    for bit in (1, 2, 4):
        if bits & bit:
            r = r + bit - 2 * bit * (lax.rem(lax.div(r, bit), 2))
    return r


def _rcopy(src, dst, ssem, rsem, dev):
    return pltpu.make_async_remote_copy(src_ref=src, dst_ref=dst, send_sem=ssem, recv_sem=rsem,
                                        device_id={"tp": dev}, device_id_type=MESH)


class _Gather:
    def __init__(self, r, buf, ssem, rsem):
        self.r, self.buf, self.ssem, self.rsem = r, buf, ssem, rsem
        self.sent = 0

    def chunk(self, owner, h):
        return self.buf.at[owner, pl.ds(32 * h, 32)]

    def send(self, rel_owner, h, to, idx, src=None):
        owner = _flip(self.r, rel_owner)
        src = self.chunk(owner, h) if src is None else src
        return _rcopy(src, self.chunk(owner, h), self.ssem.at[idx], self.rsem.at[2 * (rel_owner ^ to) + h],
                      _flip(self.r, to))

    def wait_in(self, rel_owner, h):
        owner = _flip(self.r, rel_owner)
        _rcopy(self.chunk(owner, h), self.chunk(owner, h), self.ssem.at[0], self.rsem.at[2 * rel_owner + h],
               _flip(self.r, 1)).wait_recv()

    def own(self, src=None):
        def s(h):
            return None if src is None else src.at[pl.ds(32 * h, 32)]
        self.send(0, 0, 2, 0, s(0)).start()
        self.send(0, 1, 4, 1, s(1)).start()
        self.send(0, 1, 2, 2, s(1)).start()
        self.send(0, 0, 4, 3, s(0)).start()
        self.send(0, 0, 1, 4, s(0)).start()
        self.send(0, 1, 1, 5, s(1)).start()

    def fwd1(self):
        self.wait_in(2, 0)
        self.send(2, 0, 4, 6).start()
        self.send(2, 0, 1, 7).start()
        self.wait_in(4, 1)
        self.send(4, 1, 2, 8).start()
        self.send(4, 1, 1, 9).start()

    def fwd2(self):
        self.wait_in(2, 1)
        self.send(2, 1, 1, 10).start()
        self.wait_in(4, 0)
        self.send(4, 0, 1, 11).start()

    def fwd3(self):
        self.wait_in(6, 0)
        self.send(6, 0, 1, 12).start()
        self.wait_in(6, 1)
        self.send(6, 1, 1, 13).start()

    def finish(self):
        for rel in (1, 3, 5, 7):
            for h in (0, 1):
                self.wait_in(rel, h)
        for idx in range(14):
            self.send(0, 0, 1, idx).wait_send()


def _k1(idcol, idrow, gain, tab, w, du, dres, u_out, x_out, n_out, de_out, dg_out,
        du_v, w_v, etab, dn_v, rx1, tx2, rx2, own, wc_v, u_v, n_v, nh_v, x_v, dres_v, dx_all, dgs,
        lsem, wsem, wcsem, usem, e_s, e_r, s1, r1, s2, r2, a_s, a_r, g_s, g_r):
    r = lax.axis_index("tp")
    core = lax.rem(r, 2)
    xs = lax.rem(lax.div(r, 2), 2)
    ys = lax.div(r, 4)
    cols = w.shape[1]
    n_u = cols // UC

    du_cp = [pltpu.make_async_copy(du.at[m], du_v.at[:, m], lsem.at[m]) for m in range(2)]
    for c in du_cp:
        c.start()

    def w_cp(j, slot):
        return pltpu.make_async_copy(w.at[pl.ds(pl.multiple_of(j * FB, FB), FB)], w_v.at[slot], wsem.at[slot])

    def wc_cp(i, slot):
        return pltpu.make_async_copy(w.at[:, pl.ds(pl.multiple_of(i * UC, UC), UC)], wc_v.at[slot], wcsem.at[slot])

    def u_cp(i, slot):
        return pltpu.make_async_copy(u_v.at[slot], u_out.at[:, pl.ds(pl.multiple_of(i * UC, UC), UC)], usem.at[slot])

    w_cp(0, 0).start()
    tab_cp = pltpu.make_async_copy(tab, etab.at[r], lsem.at[2])
    tab_cp.start()
    dres_cp = pltpu.make_async_copy(dres, dres_v, lsem.at[3])
    dres_cp.start()

    barrier = pltpu.get_barrier_semaphore()
    for rel in range(1, 8):
        pl.semaphore_signal(barrier, inc=1, device_id={"tp": _flip(r, rel)}, device_id_type=MESH)
    pl.semaphore_wait(barrier, 7)

    eg = _Gather(r, etab, e_s, e_r)
    eg.own(tab)
    for c in du_cp:
        c.wait()

    def rs1(j, even):
        if even:
            sib = dn_v.at[j, :, xs, 1 - core]
            far = [dn_v.at[j, :, 1 - xs, c] for c in range(2)]
            dev = [(ys * 2 + 1 - xs) * 2 + c for c in range(2)]
        else:
            sib = dn_v.at[j, ys, :, 1 - core]
            far = [dn_v.at[j, 1 - ys, :, c] for c in range(2)]
            dev = [((1 - ys) * 2 + xs) * 2 + c for c in range(2)]
        out = [_rcopy(far[c], rx1.at[j, 1 + core], s1.at[j, 1 + c], r1.at[j, 1 + core], dev[c]) for c in range(2)]
        out.append(_rcopy(sib, rx1.at[j, 0], s1.at[j, 0], r1.at[j, 0], _flip(r, 1)))
        return out

    def rs1_start(j):
        @pl.when(lax.rem(j, 2) == 0)
        def _():
            for c in rs1(j, True):
                c.start()

        @pl.when(lax.rem(j, 2) == 1)
        def _():
            for c in rs1(j, False):
                c.start()

    def other(j):
        odd = lax.rem(j, 2)
        oy = ys + (1 - 2 * ys) * (1 - odd)
        ox = xs + (1 - 2 * xs) * odd
        q = ys * (1 - odd) + xs * odd
        return oy, ox, q

    def combine(j):
        oy, ox, q = other(j)
        for s in range(3):
            _rcopy(rx1.at[j, s], rx1.at[j, s], s1.at[j, 0], r1.at[j, s], _flip(r, 1)).wait_recv()

        def total(part, qi):
            t = part.astype(F32)
            for s in range(3):
                t = t + rx1[j, s, qi].astype(F32)
            return t

        tx2[j] = total(dn_v[j, oy, ox, core], 1 - q)
        own[j] = total(dn_v[j, ys, xs, core], q)

    def rs2(j):
        oy, ox, _ = other(j)
        return _rcopy(tx2.at[j], rx2.at[j], s2.at[j], r2.at[j], (oy * 2 + ox) * 2 + core)

    def dn_step(j, carry):
        slot = lax.rem(j, 2)
        w_cp(j, slot).wait()

        @pl.when(j + 1 < NB)
        def _():
            w_cp(j + 1, 1 - slot).start()

        part = lax.dot_general(du_v[...].reshape(512, cols), w_v[slot], (((1,), (1,)), ((), ())),
                               preferred_element_type=F32)
        dn_v[j] = part.astype(BF16).reshape(2, 2, 2, 64, FB)

        @pl.when(j == 3)
        def _():
            eg.fwd1()
            for jj in range(3):
                rs1_start(jj)

        @pl.when(j > 3)
        def _():
            rs1_start(j - 1)

        @pl.when(j == 6)
        def _():
            eg.fwd2()
            wc_cp(0, 0).start()

        return carry

    lax.fori_loop(0, NB, dn_step, 0)
    tab_cp.wait()
    eg.fwd3()
    rs1_start(NB - 1)
    eg.finish()

    gf = gain[...].astype(F32)
    lanes = lax.broadcasted_iota(jnp.int32, (TB, 512), 1)

    def lookup(ids, rows):
        pick = (ids == lanes[:rows]).astype(BF16)
        return jnp.dot(pick, etab[...].reshape(512, 4096), preferred_element_type=F32)

    def n_step(b, carry):
        rows = pl.ds(pl.multiple_of(b * TB, TB), TB)
        xg = lookup(idcol[rows, :], TB)
        inv = lax.rsqrt(jnp.mean(xg * xg, axis=-1, keepdims=True) + NORM_EPS)
        n_v[rows, :] = (xg * inv * gf).astype(BF16)
        return carry

    lax.fori_loop(0, 512 // TB, n_step, 0)
    n_cp = pltpu.make_async_copy(n_v, n_out, lsem.at[0])
    n_cp.start()

    start = pl.multiple_of(r * 32, 32)
    own_ids = jnp.concatenate([idcol[pl.ds(start, 32), :], idcol[pl.ds(start + 256, 32), :]], axis=0)
    xo = lookup(own_ids, 64)
    inv_own = lax.rsqrt(jnp.mean(xo * xo, axis=-1, keepdims=True) + NORM_EPS)
    x_v[...] = xo.astype(BF16).reshape(2, 32, 4096)
    nh_v[...] = xo * inv_own
    x_cp = pltpu.make_async_copy(x_v, x_out, lsem.at[1])
    x_cp.start()

    def u_step(i, carry):
        slot = lax.rem(i, 2)
        wc_cp(i, slot).wait()

        @pl.when(i + 1 < n_u)
        def _():
            wc_cp(i + 1, 1 - slot).start()

        @pl.when(i >= 2)
        def _():
            u_cp(i - 2, slot).wait()

        u_v[slot] = jnp.dot(n_v[...], wc_v[slot], preferred_element_type=F32).astype(BF16)
        u_cp(i, slot).start()

        pair = lax.div(i, 5) - 1

        @pl.when((lax.rem(i, 5) == 0) & (i > 0))
        def _():
            combine(2 * pair)
            combine(2 * pair + 1)

        @pl.when((lax.rem(i, 5) == 1) & (i > 1))
        def _():
            rs2(2 * pair).start()
            rs2(2 * pair + 1).start()

        return carry

    lax.fori_loop(0, n_u, u_step, 0)
    combine(6)
    combine(7)
    dres_cp.wait()
    u_cp(n_u - 2, lax.rem(n_u - 2, 2)).wait()
    u_cp(n_u - 1, lax.rem(n_u - 1, 2)).wait()
    rs2(6).start()
    rs2(7).start()

    centre = jnp.zeros((64, 1), F32)
    for j in range(NB):
        sl = slice(j * FB, (j + 1) * FB)
        rs2(j).wait_recv()
        dn = own[j] + rx2[j]
        own[j] = dn
        nh = nh_v[:, sl]
        centre = centre + jnp.sum(nh * (gf[:, sl] * dn), axis=-1, keepdims=True)
        dgs[r, :, sl] = jnp.sum(dn * nh, axis=0, keepdims=True)
    centre = centre * (1.0 / 4096)
    for j in range(NB):
        sl = slice(j * FB, (j + 1) * FB)
        dr = dres_v[:, :, sl].reshape(64, FB).astype(F32)
        dx = dr + inv_own * (gf[:, sl] * own[j] - nh_v[:, sl] * centre)
        dx_all[r, :, sl] = dx.astype(BF16)

    def dg_cp(rel):
        return _rcopy(dgs.at[r], dgs.at[r], g_s.at[rel], g_r.at[r], _flip(r, rel))

    for rel in range(1, 8):
        dg_cp(rel).start()
    ag = _Gather(r, dx_all, a_s, a_r)
    ag.own()
    ag.fwd1()
    ag.fwd2()
    ag.fwd3()
    for rel in range(1, 8):
        src = _flip(r, rel)
        _rcopy(dgs.at[src], dgs.at[src], g_s.at[rel], g_r.at[src], src).wait_recv()
    tot = dgs[0]
    for k in range(1, 8):
        tot = tot + dgs[k]
    dg_out[...] = tot
    pick = (idrow[...] == r * 64 + lax.broadcasted_iota(jnp.int32, (64, 512), 0)).astype(BF16)
    ag.finish()
    de_out[...] = jnp.dot(pick, dx_all[...].reshape(512, 4096), preferred_element_type=F32)

    for rel in range(1, 8):
        dg_cp(rel).wait_send()
    for j in range(NB):
        for c in rs1(j, j % 2 == 0):
            c.wait_send()
        rs2(j).wait_send()
    n_cp.wait()
    x_cp.wait()


def solution(mesh):
    group_size = mesh.shape['tp']

    def local_step(token_ids, table_loc, gain_vec, w_loc, du_loc, dres_loc):
        num_micro, seq_len = token_ids.shape
        rows_loc, model_dim = table_loc.shape
        seq_loc = seq_len // group_size
        cols_loc = w_loc.shape[1]
        tokens = num_micro * seq_len
        du_flat = du_loc.reshape(tokens, cols_loc)
        idcol = token_ids.reshape(tokens, 1)
        idrow = token_ids.reshape(num_micro, group_size, seq_loc).transpose(1, 0, 2).reshape(1, tokens)
        vm, hb = pl.BlockSpec(memory_space=pltpu.VMEM), pl.BlockSpec(memory_space=pl.ANY)
        sd = jax.ShapeDtypeStruct
        dma = pltpu.SemaphoreType.DMA
        u_all, x_own, normed, grad_table, grad_gain = pl.pallas_call(
            _k1,
            out_shape=(sd((tokens, cols_loc), BF16), sd((num_micro, seq_loc, model_dim), BF16),
                       sd((tokens, model_dim), BF16), sd((rows_loc, model_dim), F32), sd((1, model_dim), F32)),
            in_specs=[vm, vm, vm, hb, hb, hb, hb],
            out_specs=(hb, hb, hb, vm, vm),
            scratch_shapes=[
                pltpu.VMEM((8, 2, 32, cols_loc), BF16),
                pltpu.VMEM((2, FB, cols_loc), BF16),
                pltpu.VMEM((8, 64, model_dim), BF16),
                pltpu.VMEM((NB, 2, 2, 2, 64, FB), BF16),
                pltpu.VMEM((NB, 3, 2, 64, FB), BF16),
                pltpu.VMEM((NB, 64, FB), F32),
                pltpu.VMEM((NB, 64, FB), F32),
                pltpu.VMEM((NB, 64, FB), F32),
                pltpu.VMEM((2, model_dim, UC), BF16),
                pltpu.VMEM((2, tokens, UC), BF16),
                pltpu.VMEM((tokens, model_dim), BF16),
                pltpu.VMEM((64, model_dim), F32),
                pltpu.VMEM((2, 32, model_dim), BF16),
                pltpu.VMEM((2, 32, model_dim), BF16),
                pltpu.VMEM((8, 64, model_dim), BF16),
                pltpu.VMEM((8, 1, model_dim), F32),
                dma((4,)), dma((2,)), dma((2,)), dma((2,)),
                dma((14,)), dma((16,)),
                dma((NB, 3)), dma((NB, 3)), dma((NB,)), dma((NB,)),
                dma((14,)), dma((16,)),
                dma((8,)), dma((8,)),
            ],
            compiler_params=pltpu.CompilerParams(collective_id=0, has_side_effects=True,
                                                 vmem_limit_bytes=60 * 2 ** 20),
            name="k1",
        )(idcol, idrow, gain_vec.reshape(1, model_dim), table_loc, w_loc,
          du_loc.reshape(num_micro, group_size, seq_loc, cols_loc), dres_loc)
        grad_w = lax.dot_general(normed, du_flat, (((0,), (0,)), ((), ())), preferred_element_type=F32)
        return u_all.reshape(num_micro, seq_len, cols_loc), x_own, grad_table, grad_w, grad_gain.reshape(model_dim)

    return jax.shard_map(local_step, mesh=mesh,
                         in_specs=(P('dp', None), P('tp', None), P(None), P(None, 'tp'), P('dp', None, 'tp'), P('dp', 'tp', None)),
                         out_specs=(P('dp', None, 'tp'), P('dp', 'tp', None), P(('dp', 'tp'), None), P(None, ('dp', 'tp')), P('dp')),
                         check_vma=False)
```

```python
import functools

import jax
import jax.numpy as jnp
from jax import lax
from jax.experimental import pallas as pl
from jax.experimental.pallas import tpu as pltpu
from jax.sharding import PartitionSpec as P

NORM_EPS = 1e-6
MESH = pl.DeviceIdType.MESH
F32 = jnp.float32
BF16 = jnp.bfloat16
FB = 512
NB = 8
UC = 256
TB = 128
WS = 3
CS = 4


def _flip(r, bits):
    for bit in (1, 2, 4):
        if bits & bit:
            r = r + bit - 2 * bit * (lax.rem(lax.div(r, bit), 2))
    return r


def _rcopy(src, dst, ssem, rsem, dev):
    return pltpu.make_async_remote_copy(src_ref=src, dst_ref=dst, send_sem=ssem, recv_sem=rsem,
                                        device_id={"tp": dev}, device_id_type=MESH)


class _Gather:
    def __init__(self, r, chunk, ssem, rsem):
        self.r, self.chunk, self.ssem, self.rsem = r, chunk, ssem, rsem

    def send(self, rel_owner, h, to, idx, src=None):
        owner = _flip(self.r, rel_owner)
        src = self.chunk(owner, h) if src is None else src
        return _rcopy(src, self.chunk(owner, h), self.ssem.at[idx], self.rsem.at[2 * (rel_owner ^ to) + h],
                      _flip(self.r, to))

    def wait_in(self, rel_owner, h):
        owner = _flip(self.r, rel_owner)
        _rcopy(self.chunk(owner, h), self.chunk(owner, h), self.ssem.at[0], self.rsem.at[2 * rel_owner + h],
               _flip(self.r, 1)).wait_recv()

    def own(self, src=None):
        def s(h):
            return None if src is None else src.at[pl.ds(32 * h, 32)]
        self.send(0, 0, 2, 0, s(0)).start()
        self.send(0, 1, 4, 1, s(1)).start()
        self.send(0, 1, 2, 2, s(1)).start()
        self.send(0, 0, 4, 3, s(0)).start()
        self.send(0, 0, 1, 4, s(0)).start()
        self.send(0, 1, 1, 5, s(1)).start()

    def fwd1(self):
        self.wait_in(2, 0)
        self.send(2, 0, 4, 6).start()
        self.send(2, 0, 1, 7).start()
        self.wait_in(4, 1)
        self.send(4, 1, 2, 8).start()
        self.send(4, 1, 1, 9).start()

    def fwd2(self):
        self.wait_in(2, 1)
        self.send(2, 1, 1, 10).start()
        self.wait_in(4, 0)
        self.send(4, 0, 1, 11).start()

    def fwd3(self):
        self.wait_in(6, 0)
        self.send(6, 0, 1, 12).start()
        self.wait_in(6, 1)
        self.send(6, 1, 1, 13).start()

    def finish(self):
        for rel in (1, 3, 5, 7):
            for h in (0, 1):
                self.wait_in(rel, h)
        for idx in range(14):
            self.send(0, 0, 1, idx).wait_send()


def _k1(ids, gain, tab, w, du, dres, u_out, x_out, n_out, de_out, dg_out,
        du_v, w_v, etab, dn_v, rx1, tx2, rx2, own, wc_v, u_v, n_v, nh_v, x_v, dres_v, dx_all, dgs,
        lsem, wsem, wcsem, usem, e_s, e_r, s1, r1, s2, r2, a_s, a_r, g_s, g_r):
    r = lax.axis_index("tp")
    core = lax.rem(r, 2)
    xs = lax.rem(lax.div(r, 2), 2)
    ys = lax.div(r, 4)
    cols = w.shape[1]
    n_u = cols // UC

    du_cp = [pltpu.make_async_copy(du.at[m], du_v.at[:, m], lsem.at[m]) for m in range(2)]
    for c in du_cp:
        c.start()

    def w_cp(j, slot):
        return pltpu.make_async_copy(w.at[pl.ds(pl.multiple_of(j * FB, FB), FB)], w_v.at[slot], wsem.at[slot])

    def wc_cp(i, slot):
        return pltpu.make_async_copy(w.at[:, pl.ds(pl.multiple_of(i * UC, UC), UC)], wc_v.at[slot], wcsem.at[slot])

    def u_cp(i, slot):
        return pltpu.make_async_copy(u_v.at[slot], u_out.at[:, pl.ds(pl.multiple_of(i * UC, UC), UC)], usem.at[slot])

    for k in range(WS - 1):
        w_cp(k, k).start()
    tab_cp = pltpu.make_async_copy(tab, etab.at[r], lsem.at[2])
    tab_cp.start()
    dres_cp = pltpu.make_async_copy(dres, dres_v, lsem.at[3])
    dres_cp.start()

    barrier = pltpu.get_barrier_semaphore()
    for rel in range(1, 8):
        pl.semaphore_signal(barrier, inc=1, device_id={"tp": _flip(r, rel)}, device_id_type=MESH)
    pl.semaphore_wait(barrier, 7)

    eg = _Gather(r, lambda owner, h: etab.at[owner, pl.ds(32 * h, 32)], e_s, e_r)
    eg.own(tab)
    for c in du_cp:
        c.wait()

    def rs1(j, even):
        if even:
            sib = dn_v.at[j, :, xs, 1 - core]
            far = [dn_v.at[j, :, 1 - xs, c] for c in range(2)]
            dev = [(ys * 2 + 1 - xs) * 2 + c for c in range(2)]
        else:
            sib = dn_v.at[j, ys, :, 1 - core]
            far = [dn_v.at[j, 1 - ys, :, c] for c in range(2)]
            dev = [((1 - ys) * 2 + xs) * 2 + c for c in range(2)]
        out = [_rcopy(far[c], rx1.at[j, 1 + core], s1.at[j, 1 + c], r1.at[j, 1 + core], dev[c]) for c in range(2)]
        out.append(_rcopy(sib, rx1.at[j, 0], s1.at[j, 0], r1.at[j, 0], _flip(r, 1)))
        return out

    def rs1_start(j):
        @pl.when(lax.rem(j, 2) == 0)
        def _():
            for c in rs1(j, True):
                c.start()

        @pl.when(lax.rem(j, 2) == 1)
        def _():
            for c in rs1(j, False):
                c.start()

    def other(j):
        odd = lax.rem(j, 2)
        oy = ys + (1 - 2 * ys) * (1 - odd)
        ox = xs + (1 - 2 * xs) * odd
        q = ys * (1 - odd) + xs * odd
        return oy, ox, q

    def combine(j):
        oy, ox, q = other(j)
        for s in range(3):
            _rcopy(rx1.at[j, s], rx1.at[j, s], s1.at[j, 0], r1.at[j, s], _flip(r, 1)).wait_recv()

        def total(part, qi):
            t = part.astype(F32)
            for s in range(3):
                t = t + rx1[j, s, qi].astype(F32)
            return t

        tx2[j] = total(dn_v[j, oy, ox, core], 1 - q)
        own[j] = total(dn_v[j, ys, xs, core], q)

    def rs2(j):
        oy, ox, _ = other(j)
        return _rcopy(tx2.at[j], rx2.at[j], s2.at[j], r2.at[j], (oy * 2 + ox) * 2 + core)

    def dn_step(j, carry):
        slot = lax.rem(j, WS)
        w_cp(j, slot).wait()

        @pl.when(j + WS - 1 < NB)
        def _():
            w_cp(j + WS - 1, lax.rem(j + WS - 1, WS)).start()

        part = lax.dot_general(du_v[...].reshape(512, cols), w_v[slot], (((1,), (1,)), ((), ())),
                               preferred_element_type=F32)
        dn_v[j] = part.astype(BF16).reshape(2, 2, 2, 64, FB)

        @pl.when(j == 3)
        def _():
            eg.fwd1()
            for jj in range(3):
                rs1_start(jj)

        @pl.when(j > 3)
        def _():
            rs1_start(j - 1)

        @pl.when(j == 6)
        def _():
            eg.fwd2()
            for k in range(CS - 1):
                wc_cp(k, k).start()

        return carry

    lax.fori_loop(0, NB, dn_step, 0)
    tab_cp.wait()
    eg.fwd3()
    rs1_start(NB - 1)
    eg.finish()

    gf = gain[...].astype(F32).reshape(1, 4096)

    def one_hot(first, rows, tok):
        return (tok == first + lax.broadcasted_iota(jnp.int32, (rows, tok.shape[1]), 0)).astype(BF16)

    def lookup(pick_t):
        return lax.dot_general(pick_t, etab[...].reshape(512, 4096), (((0,), (0,)), ((), ())),
                               preferred_element_type=F32)

    for b in range(512 // TB):
        rows = slice(b * TB, (b + 1) * TB)
        col = b * TB % 256
        xg = lookup(one_hot(0, 512, ids[b * TB // 256:b * TB // 256 + 1, col:col + TB]))
        inv = lax.rsqrt(jnp.mean(xg * xg, axis=-1, keepdims=True) + NORM_EPS)
        n_v[rows, :] = (xg * inv * gf).astype(BF16)

    n_cp = pltpu.make_async_copy(n_v, n_out, lsem.at[0])
    n_cp.start()

    mine = (lax.broadcasted_iota(jnp.int32, (32, 256), 1) ==
            r * 32 + lax.broadcasted_iota(jnp.int32, (32, 256), 0)).astype(BF16)
    pick_own = jnp.concatenate(
        [lax.dot_general(mine, one_hot(0, 512, ids[m:m + 1, :]), (((1,), (1,)), ((), ())), preferred_element_type=F32)
         for m in range(2)], axis=0).astype(BF16)
    xo = jnp.dot(pick_own, etab[...].reshape(512, 4096), preferred_element_type=F32)
    inv_own = lax.rsqrt(jnp.mean(xo * xo, axis=-1, keepdims=True) + NORM_EPS)
    x_v[...] = xo.astype(BF16).reshape(2, 32, 4096)
    nh_v[...] = xo * inv_own
    x_cp = pltpu.make_async_copy(x_v, x_out, lsem.at[1])
    x_cp.start()

    def u_step(i, carry):
        slot = lax.rem(i, 2)
        wslot = lax.rem(i, CS)
        wc_cp(i, wslot).wait()

        @pl.when(i + CS - 1 < n_u)
        def _():
            wc_cp(i + CS - 1, lax.rem(i + CS - 1, CS)).start()

        @pl.when(i >= 2)
        def _():
            u_cp(i - 2, slot).wait()

        u_v[slot] = jnp.dot(n_v[...], wc_v[wslot], preferred_element_type=F32).astype(BF16)
        u_cp(i, slot).start()

        pair = lax.div(i, 5)

        @pl.when(lax.rem(i, 5) == 0)
        def _():
            combine(2 * pair)
            combine(2 * pair + 1)

        @pl.when(lax.rem(i, 5) == 1)
        def _():
            rs2(2 * pair).start()
            rs2(2 * pair + 1).start()

        return carry

    lax.fori_loop(0, n_u, u_step, 0)
    dres_cp.wait()
    u_cp(n_u - 2, lax.rem(n_u - 2, 2)).wait()
    u_cp(n_u - 1, lax.rem(n_u - 1, 2)).wait()

    centre = jnp.zeros((64, 1), F32)
    for j in range(NB):
        sl = slice(j * FB, (j + 1) * FB)
        rs2(j).wait_recv()
        dn = own[j] + rx2[j]
        own[j] = dn
        nh = nh_v[:, sl]
        centre = centre + jnp.sum(nh * (gf[:, sl] * dn), axis=-1, keepdims=True)
        dgs[r, :, sl] = jnp.sum(dn * nh, axis=0, keepdims=True)
    centre = centre * (1.0 / 4096)
    for j in range(NB):
        sl = slice(j * FB, (j + 1) * FB)
        dr = dres_v[:, :, sl].reshape(64, FB).astype(F32)
        dx = dr + inv_own * (gf[:, sl] * own[j] - nh_v[:, sl] * centre)
        for m in range(2):
            dx_all[m, r, :, sl] = dx[32 * m:32 * m + 32].astype(BF16)

    def dg_cp(rel):
        return _rcopy(dgs.at[r], dgs.at[r], g_s.at[rel], g_r.at[r], _flip(r, rel))

    for rel in range(1, 8):
        dg_cp(rel).start()
    ag = _Gather(r, lambda owner, h: dx_all.at[h, owner], a_s, a_r)
    ag.own()
    ag.fwd1()
    ag.fwd2()
    ag.fwd3()
    for rel in range(1, 8):
        src = _flip(r, rel)
        _rcopy(dgs.at[src], dgs.at[src], g_s.at[rel], g_r.at[src], src).wait_recv()
    tot = dgs[0]
    for k in range(1, 8):
        tot = tot + dgs[k]
    dg_out[...] = tot
    pick = jnp.concatenate([one_hot(r * 64, 64, ids[m:m + 1, :]) for m in range(2)], axis=1)
    ag.finish()
    de_out[...] = jnp.dot(pick, dx_all[...].reshape(512, 4096), preferred_element_type=F32)

    for rel in range(1, 8):
        dg_cp(rel).wait_send()
    for j in range(NB):
        for c in rs1(j, j % 2 == 0):
            c.wait_send()
        rs2(j).wait_send()
    n_cp.wait()
    x_cp.wait()


def _k2(n_ref, du_ref, u_ref, x_ref, de_ref, dg_ref, dw_out, u_out, x_out, de_out, dg_out):
    dw_out[...] = lax.dot_general(n_ref[...], du_ref[...], (((0,), (0,)), ((), ())), preferred_element_type=F32)
    u_out[...] = u_ref[...]
    x_out[...] = x_ref[...]
    de_out[...] = de_ref[...]
    dg_out[...] = dg_ref[...]


def solution(mesh):
    group_size = mesh.shape['tp']

    def local_step(token_ids, table_loc, gain_vec, w_loc, du_loc, dres_loc):
        num_micro, seq_len = token_ids.shape
        rows_loc, model_dim = table_loc.shape
        seq_loc = seq_len // group_size
        cols_loc = w_loc.shape[1]
        tokens = num_micro * seq_len
        du_flat = du_loc.reshape(tokens, cols_loc)
        vm, hb = pl.BlockSpec(memory_space=pltpu.VMEM), pl.BlockSpec(memory_space=pl.ANY)
        sd = jax.ShapeDtypeStruct
        dma = pltpu.SemaphoreType.DMA
        u_all, x_own, normed, grad_table, grad_gain = pl.pallas_call(
            _k1,
            out_shape=(sd((tokens, cols_loc), BF16), sd((num_micro, seq_loc, model_dim), BF16),
                       sd((tokens, model_dim), BF16), sd((rows_loc, model_dim), F32), sd((1, model_dim), F32)),
            in_specs=[vm, vm, hb, hb, hb, hb],
            out_specs=(hb, hb, hb, vm, vm),
            scratch_shapes=[
                pltpu.VMEM((8, 2, 32, cols_loc), BF16),
                pltpu.VMEM((WS, FB, cols_loc), BF16),
                pltpu.VMEM((8, 64, model_dim), BF16),
                pltpu.VMEM((NB, 2, 2, 2, 64, FB), BF16),
                pltpu.VMEM((NB, 3, 2, 64, FB), BF16),
                pltpu.VMEM((NB, 64, FB), F32),
                pltpu.VMEM((NB, 64, FB), F32),
                pltpu.VMEM((NB, 64, FB), F32),
                pltpu.VMEM((CS, model_dim, UC), BF16),
                pltpu.VMEM((2, tokens, UC), BF16),
                pltpu.VMEM((tokens, model_dim), BF16),
                pltpu.VMEM((64, model_dim), F32),
                pltpu.VMEM((2, 32, model_dim), BF16),
                pltpu.VMEM((2, 32, model_dim), BF16),
                pltpu.VMEM((2, 8, 32, model_dim), BF16),
                pltpu.VMEM((8, 1, model_dim), F32),
                dma((4,)), dma((WS,)), dma((CS,)), dma((2,)),
                dma((14,)), dma((16,)),
                dma((NB, 3)), dma((NB, 3)), dma((NB,)), dma((NB,)),
                dma((14,)), dma((16,)),
                dma((8,)), dma((8,)),
            ],
            compiler_params=pltpu.CompilerParams(collective_id=0, has_side_effects=True,
                                                 vmem_limit_bytes=60 * 2 ** 20),
            name="k1",
        )(token_ids, gain_vec, table_loc, w_loc,
          du_loc.reshape(num_micro, group_size, seq_loc, cols_loc), dres_loc)
        steps = 16
        fb, ub = model_dim // steps, tokens // steps
        blk = pl.BlockSpec
        io = [blk((ub, cols_loc), lambda i: (i, 0)), blk((num_micro, seq_loc, fb), lambda i: (0, 0, i)),
              blk((rows_loc, fb), lambda i: (0, i)), blk((1, fb), lambda i: (0, i))]
        grad_w, u_all, x_own, grad_table, grad_gain = pl.pallas_call(
            _k2,
            grid=(steps,),
            out_shape=(sd((model_dim, cols_loc), F32), sd((tokens, cols_loc), BF16),
                       sd((num_micro, seq_loc, model_dim), BF16), sd((rows_loc, model_dim), F32),
                       sd((1, model_dim), F32)),
            in_specs=[blk((tokens, fb), lambda i: (0, i)), blk((tokens, cols_loc), lambda i: (0, 0))] + io,
            out_specs=[blk((fb, cols_loc), lambda i: (i, 0))] + io,
            compiler_params=pltpu.CompilerParams(dimension_semantics=("arbitrary",), vmem_limit_bytes=60 * 2 ** 20),
            name="k2",
        )(normed, du_flat, u_all, x_own, grad_table, grad_gain)
        return u_all.reshape(num_micro, seq_len, cols_loc), x_own, grad_table, grad_w, grad_gain.reshape(model_dim)

    return jax.shard_map(local_step, mesh=mesh,
                         in_specs=(P('dp', None), P('tp', None), P(None), P(None, 'tp'), P('dp', None, 'tp'), P('dp', 'tp', None)),
                         out_specs=(P('dp', None, 'tp'), P('dp', 'tp', None), P(('dp', 'tp'), None), P(None, ('dp', 'tp')), P('dp')),
                         check_vma=False)
```

```python
import functools

import jax
import jax.numpy as jnp
from jax import lax
from jax.experimental import pallas as pl
from jax.experimental.pallas import tpu as pltpu
from jax.sharding import PartitionSpec as P

NORM_EPS = 1e-6
MESH = pl.DeviceIdType.MESH
F32 = jnp.float32
BF16 = jnp.bfloat16
FB = 512
NB = 8
UC = 512
TB = 128
DF = 256
RS = 4
WS = 3
CS = 3


def _flip(r, bits):
    for bit in (1, 2, 4):
        if bits & bit:
            r = r + bit - 2 * bit * (lax.rem(lax.div(r, bit), 2))
    return r


def _rcopy(src, dst, ssem, rsem, dev, dp=None):
    return pltpu.make_async_remote_copy(src_ref=src, dst_ref=dst, send_sem=ssem, recv_sem=rsem,
                                        device_id={"tp": dev} if dp is None else {"dp": dp, "tp": dev},
                                        device_id_type=MESH)


class _Gather:
    def __init__(self, r, chunk, ssem, rsem):
        self.r, self.chunk, self.ssem, self.rsem = r, chunk, ssem, rsem

    def send(self, rel_owner, h, to, idx):
        owner = _flip(self.r, rel_owner)
        return _rcopy(self.chunk(owner, h), self.chunk(owner, h), self.ssem.at[idx], self.rsem.at[2 * (rel_owner ^ to) + h],
                      _flip(self.r, to))

    def wait_in(self, rel_owner, h):
        owner = _flip(self.r, rel_owner)
        _rcopy(self.chunk(owner, h), self.chunk(owner, h), self.ssem.at[0], self.rsem.at[2 * rel_owner + h],
               _flip(self.r, 1)).wait_recv()

    def own(self):
        self.send(0, 0, 2, 0).start()
        self.send(0, 1, 4, 1).start()
        self.send(0, 1, 2, 2).start()
        self.send(0, 0, 4, 3).start()
        self.send(0, 0, 1, 4).start()
        self.send(0, 1, 1, 5).start()

    def fwd1(self):
        self.wait_in(2, 0)
        self.send(2, 0, 4, 6).start()
        self.send(2, 0, 1, 7).start()
        self.wait_in(4, 1)
        self.send(4, 1, 2, 8).start()
        self.send(4, 1, 1, 9).start()

    def fwd2(self):
        self.wait_in(2, 1)
        self.send(2, 1, 1, 10).start()
        self.wait_in(4, 0)
        self.send(4, 0, 1, 11).start()

    def fwd3(self):
        self.wait_in(6, 0)
        self.send(6, 0, 1, 12).start()
        self.wait_in(6, 1)
        self.send(6, 1, 1, 13).start()

    def finish(self):
        for rel in (1, 3, 5, 7):
            for h in (0, 1):
                self.wait_in(rel, h)
        for idx in range(14):
            self.send(0, 0, 1, idx).wait_send()


class _TableGather:
    def __init__(self, r, p, buf, tab, ssem, rsem):
        self.r, self.p, self.buf, self.tab, self.ssem, self.rsem = r, p, buf, tab, ssem, rsem

    def rows(self, k):
        return pl.ds(pl.multiple_of(16 * (k + self.p * (3 - 2 * k)), 16), 16)

    def own(self):
        for n, (to, k) in enumerate(((2, 0), (4, 2), (2, 1), (4, 3))):
            _rcopy(self.tab.at[self.rows(k)], self.buf.at[self.r, self.rows(k)], self.ssem.at[n],
                   self.rsem.at[2 * to + k], _flip(self.r, to)).start()
        _rcopy(self.tab, self.buf.at[self.r], self.ssem.at[4], self.rsem.at[0], _flip(self.r, 1)).start()

    def wait_in(self, rel, k):
        src = self.buf.at[_flip(self.r, rel), self.rows(k)]
        _rcopy(src, src, self.ssem.at[0], self.rsem.at[2 * rel + k], _flip(self.r, 1)).wait_recv()

    def fwd(self, rel, k, to, idx):
        src = self.buf.at[_flip(self.r, rel), self.rows(k)]
        _rcopy(src, src, self.ssem.at[idx], self.rsem.at[2 * (rel ^ to) + k], _flip(self.r, to)).start()

    def twin(self, rel, k, idx):
        src = self.buf.at[_flip(self.r, rel), self.rows(k)]
        _rcopy(src, src, self.ssem.at[idx], self.rsem.at[2 * rel + 3 - k], self.r, 1 - self.p).start()

    def block(self, rel, idx, start):
        src = self.buf.at[_flip(self.r, rel)]
        c = _rcopy(src, src, self.ssem.at[idx], self.rsem.at[rel // 2], _flip(self.r, 1))
        if start:
            c.start()
        else:
            c.wait_recv()

    def relay(self, n):
        for rel, k, to in ((2, n, 4), (4, 2 + n, 2)):
            self.wait_in(rel, k)
            self.fwd(rel, k, to, 5 + 2 * n + (rel // 4))
            self.twin(rel, k, 9 + 2 * n + (rel // 4))

    def blocks(self):
        for n, (rel, ks) in enumerate(((2, (2, 3)), (4, (0, 1)), (6, (0, 1, 2, 3)))):
            for k in ks:
                self.wait_in(rel, k)
            self.block(rel, 13 + n, True)

    def finish(self):
        _rcopy(self.tab, self.buf.at[self.r], self.ssem.at[4], self.rsem.at[0], _flip(self.r, 1)).wait_recv()
        for n, rel in enumerate((2, 4, 6)):
            self.block(rel, 13 + n, False)
        small = self.buf.at[self.r, self.rows(0)]
        for n in range(16):
            src = self.buf.at[self.r] if n in (4, 13, 14, 15) else small
            _rcopy(src, src, self.ssem.at[n], self.rsem.at[0], _flip(self.r, 1)).wait_send()


def _k1(ids, gain, tab, w, du, dres, u_out, x_out, n_out, de_out, dg_out,
        du_v, w_v, etab, dn_v, rx1, tx2, rx2, own, wc_v, u_v, n_v, nh_v, inv_v, x_v, dres_v, dx_all, dgs,
        lsem, wsem, wcsem, usem, e_s, e_r, s1, r1, s2, r2, a_s, a_r, g_s, g_r):
    r = lax.axis_index("tp")
    p = lax.axis_index("dp")
    core = lax.rem(r, 2)
    xs = lax.rem(lax.div(r, 2), 2)
    ys = lax.div(r, 4)
    cols = w.shape[1]
    n_u = cols // UC
    rest = cols - n_u * UC

    du_cp = pltpu.make_async_copy(du, du_v, lsem.at[0])
    du_cp.start()

    def w_cp(j, slot):
        return pltpu.make_async_copy(w.at[pl.ds(pl.multiple_of(j * FB, FB), FB)], w_v.at[slot], wsem.at[slot])

    def wc_cp(i, slot):
        return pltpu.make_async_copy(w.at[:, pl.ds(pl.multiple_of(i * UC, UC), UC)], wc_v.at[slot], wcsem.at[slot])

    def wr_cp():
        return pltpu.make_async_copy(w.at[:, pl.ds(n_u * UC, rest)], wc_v.at[n_u % CS, :, pl.ds(0, rest)],
                                     wcsem.at[n_u % CS])

    def ur_cp():
        return pltpu.make_async_copy(u_v.at[n_u % 2, :, pl.ds(0, rest)], u_out.at[:, pl.ds(n_u * UC, rest)],
                                     usem.at[n_u % 2])

    def u_cp(i, slot):
        return pltpu.make_async_copy(u_v.at[slot], u_out.at[:, pl.ds(pl.multiple_of(i * UC, UC), UC)], usem.at[slot])

    for k in range(WS - 1):
        w_cp(k, k).start()
    tab_cp = pltpu.make_async_copy(tab, etab.at[r], lsem.at[2])
    tab_cp.start()
    dres_cp = pltpu.make_async_copy(dres, dres_v, lsem.at[3])
    dres_cp.start()

    barrier = pltpu.get_barrier_semaphore()
    for rel in range(1, 8):
        pl.semaphore_signal(barrier, inc=1, device_id={"tp": _flip(r, rel)}, device_id_type=MESH)
    pl.semaphore_signal(barrier, inc=1, device_id={"dp": 1 - p, "tp": r}, device_id_type=MESH)
    pl.semaphore_wait(barrier, 8)

    eg = _TableGather(r, p, etab, tab, e_s, e_r)
    eg.own()
    du_cp.wait()

    def rs1(j, m, even):
        if even:
            sib = dn_v.at[j, m, :, xs, 1 - core]
            far = [dn_v.at[j, m, :, 1 - xs, c] for c in range(2)]
            dev = [(ys * 2 + 1 - xs) * 2 + c for c in range(2)]
        else:
            sib = dn_v.at[j, m, ys, :, 1 - core]
            far = [dn_v.at[j, m, 1 - ys, :, c] for c in range(2)]
            dev = [((1 - ys) * 2 + xs) * 2 + c for c in range(2)]
        out = [_rcopy(far[c], rx1.at[j, m, 1 + core], s1.at[j, m, 1 + c], r1.at[j, m, 1 + core], dev[c])
               for c in range(2)]
        out.append(_rcopy(sib, rx1.at[j, m, 0], s1.at[j, m, 0], r1.at[j, m, 0], _flip(r, 1)))
        return out

    def rs1_start(j, m):
        if isinstance(j, int):
            for c in rs1(j, m, j % 2 == 0):
                c.start()
            return

        @pl.when(lax.rem(j, 2) == 0)
        def _():
            for c in rs1(j, m, True):
                c.start()

        @pl.when(lax.rem(j, 2) == 1)
        def _():
            for c in rs1(j, m, False):
                c.start()

    def combine(m, pair):
        for j in (2 * pair, 2 * pair + 1):
            oy, ox, q = (1 - ys, xs, ys) if j % 2 == 0 else (ys, 1 - xs, xs)
            for n in range(3):
                _rcopy(rx1.at[j, m, n], rx1.at[j, m, n], s1.at[j, m, 0], r1.at[j, m, n], _flip(r, 1)).wait_recv()

            def total(part, qi):
                t = part.astype(F32)
                for n in range(3):
                    t = t + rx1[j, m, n, qi].astype(F32)
                return t

            tx2[m, j] = total(dn_v[j, m, oy, ox, core], 1 - q)
            own[m, j] = total(dn_v[j, m, ys, xs, core], q)

    def rs2(m, j):
        oy, ox = (1 - ys, xs) if j % 2 == 0 else (ys, 1 - xs)
        return _rcopy(tx2.at[m, j], rx2.at[m, j], s2.at[m, j], r2.at[m, j], (oy * 2 + ox) * 2 + core)

    def rs2_start(m, pair):
        rs2(m, 2 * pair).start()
        rs2(m, 2 * pair + 1).start()

    def dn_step(j, carry):
        slot = lax.rem(j, WS)
        w_cp(j, slot).wait()

        @pl.when(j + WS - 1 < NB)
        def _():
            w_cp(j + WS - 1, lax.rem(j + WS - 1, WS)).start()

        part = lax.dot_general(du_v[...], w_v[slot], (((1,), (1,)), ((), ())),
                               preferred_element_type=F32)
        dn_v[j] = part.astype(BF16).reshape(2, 2, 2, 2, 32, FB)

        for n in range(2):
            @pl.when(j == n)
            def _():
                eg.relay(n)

        @pl.when(j == 2)
        def _():
            rs1_start(0, 0)

        @pl.when(j > 1)
        def _():
            rs1_start(j - 1, 0)

        @pl.when(j > 3)
        def _():
            rs1_start(j - 4, 1)

        @pl.when(j == 4)
        def _():
            eg.blocks()

        @pl.when(j == NB - 2)
        def _():
            for k in range(CS - 1):
                wc_cp(k, k).start()

        return carry

    lax.fori_loop(0, NB, dn_step, 0)
    tab_cp.wait()
    rs1_start(7, 0)
    rs1_start(4, 1)
    combine(0, 0)
    combine(0, 1)
    eg.finish()

    gf = gain[...].astype(F32).reshape(1, 4096)

    def one_hot(first, rows, tok):
        return (tok == first + lax.broadcasted_iota(jnp.int32, (rows, tok.shape[1]), 0)).astype(BF16)

    def lookup(pick_t):
        return lax.dot_general(pick_t, etab[...].reshape(512, 4096), (((0,), (0,)), ((), ())),
                               preferred_element_type=F32)

    for b in range(512 // TB):
        rows = slice(b * TB, (b + 1) * TB)
        col = b * TB % 256
        xg = lookup(one_hot(0, 512, ids[b * TB // 256:b * TB // 256 + 1, col:col + TB]))
        inv = lax.rsqrt(jnp.mean(xg * xg, axis=-1, keepdims=True) + NORM_EPS)
        n_v[rows, :] = (xg * inv * gf).astype(BF16)
        if b == 0:
            rs2_start(0, 0)
            rs2_start(0, 1)

    n_cp = pltpu.make_async_copy(n_v, n_out, lsem.at[0])
    n_cp.start()

    mine = (lax.broadcasted_iota(jnp.int32, (32, 256), 1) ==
            r * 32 + lax.broadcasted_iota(jnp.int32, (32, 256), 0)).astype(BF16)
    pick_own = jnp.concatenate(
        [lax.dot_general(mine, one_hot(0, 512, ids[m:m + 1, :]), (((1,), (1,)), ((), ())), preferred_element_type=F32)
         for m in range(2)], axis=0).astype(BF16)
    xo = jnp.dot(pick_own, etab[...].reshape(512, 4096), preferred_element_type=F32)
    inv_own = lax.rsqrt(jnp.mean(xo * xo, axis=-1, keepdims=True) + NORM_EPS)
    x_v[...] = xo.astype(BF16).reshape(2, 32, 4096)
    nh_v[...] = xo * inv_own
    inv_v[...] = jnp.broadcast_to(inv_own, (64, 128))
    x_cp = pltpu.make_async_copy(x_v, x_out, lsem.at[1])
    x_cp.start()

    def dx_of(m):
        rows = slice(32 * m, 32 * m + 32)
        centre = jnp.zeros((32, 1), F32)
        for j in range(NB):
            sl = slice(j * FB, (j + 1) * FB)
            rs2(m, j).wait_recv()
            dn = own[m, j] + rx2[m, j]
            own[m, j] = dn
            nh = nh_v[rows, sl]
            centre = centre + jnp.sum(nh * (gf[:, sl] * dn), axis=-1, keepdims=True)
            part = jnp.sum(dn * nh, axis=0, keepdims=True)
            dgs[r, :, sl] = part if m == 0 else dgs[r, :, sl] + part
        centre = centre * (1.0 / 4096)
        for j in range(NB):
            sl = slice(j * FB, (j + 1) * FB)
            dr = dres_v[m, :, sl].astype(F32)
            dx = dr + inv_v[rows, 0:1] * (gf[:, sl] * own[m, j] - nh_v[rows, sl] * centre)
            dx_all[m, r, :, sl] = dx.astype(BF16)

    def dx_gather(m):
        return _Gather(r, lambda owner, h: dx_all.at[m, owner, pl.ds(16 * h, 16)], a_s.at[m], a_r.at[m])

    ag = [dx_gather(m) for m in range(2)]
    dres_cp.wait()
    combine(0, 2)
    events = {
        0: lambda: rs2_start(0, 2),
        1: lambda: (rs1_start(5, 1), combine(0, 3)),
        2: lambda: (rs2_start(0, 3), rs1_start(6, 1), rs1_start(7, 1), combine(1, 0)),
        3: lambda: (rs2_start(1, 0), combine(1, 1)),
        4: lambda: (rs2_start(1, 1), combine(1, 2)),
        5: lambda: (rs2_start(1, 2), dx_of(0)),
        6: lambda: (ag[0].own(), combine(1, 3)),
        7: lambda: rs2_start(1, 3),
    }

    def u_step(i, carry):
        slot = lax.rem(i, 2)
        wslot = lax.rem(i, CS)
        wc_cp(i, wslot).wait()

        @pl.when(i + CS - 1 < n_u)
        def _():
            wc_cp(i + CS - 1, lax.rem(i + CS - 1, CS)).start()

        @pl.when(i + CS - 1 == n_u)
        def _():
            wr_cp().start()

        @pl.when(i >= 2)
        def _():
            u_cp(i - 2, slot).wait()

        u_v[slot] = jnp.dot(n_v[...], wc_v[wslot], preferred_element_type=F32).astype(BF16)
        u_cp(i, slot).start()

        for at, event in events.items():
            pl.when(i == at)(lambda event=event: (event(), None)[1])

        return carry

    lax.fori_loop(0, n_u, u_step, 0)
    wr_cp().wait()
    u_cp(n_u - 2, n_u % 2).wait()
    u_v[n_u % 2, :, :rest] = jnp.dot(n_v[...], wc_v[n_u % CS, :, :rest], preferred_element_type=F32).astype(BF16)
    ur_cp().start()
    ag[0].fwd1()
    ag[0].fwd2()
    dx_of(1)
    def dg_cp(rel):
        return _rcopy(dgs.at[r], dgs.at[r], g_s.at[rel], g_r.at[r], _flip(r, rel))

    ag[1].own()
    for rel in range(1, 8):
        dg_cp(rel).start()
    ag[0].fwd3()
    ag[1].fwd1()
    u_cp(n_u - 1, (n_u - 1) % 2).wait()
    ur_cp().wait()
    ag[0].finish()
    ag[1].fwd2()
    ag[1].fwd3()
    for rel in range(1, 8):
        src = _flip(r, rel)
        _rcopy(dgs.at[src], dgs.at[src], g_s.at[rel], g_r.at[src], src).wait_recv()
    tot = dgs[0]
    for k in range(1, 8):
        tot = tot + dgs[k]
    dg_out[...] = tot
    pick = jnp.concatenate([one_hot(r * 64, 64, ids[m:m + 1, :]) for m in range(2)], axis=1)
    ag[1].finish()
    de_out[...] = jnp.dot(pick, dx_all[...].reshape(512, 4096), preferred_element_type=F32)

    for rel in range(1, 8):
        dg_cp(rel).wait_send()
    for m in range(2):
        for j in range(NB):
            for c in rs1(j, m, j % 2 == 0):
                c.wait_send()
            rs2(m, j).wait_send()
    n_cp.wait()
    x_cp.wait()


def _k2(n_in, du_in, u_in, x_in, de_in, dg_in, dw_out, u_out, x_out, de_out, dg_out,
        n_v, du_v, ring, u_v, x_v, de_v, dg_v, lsem, psem, qsem, osem):
    steps = n_in.shape[1] // DF
    half = 9 * 256
    cols = du_in.shape[1]
    parts = (pl.ds(0, half), pl.ds(half, cols - half))
    cp = pltpu.make_async_copy
    loads = [cp(n_in.at[:, pl.ds(0, DF)], n_v.at[:, pl.ds(0, DF)], lsem.at[0]),
             cp(du_in.at[:, parts[0]], du_v.at[:, parts[0]], lsem.at[1]),
             cp(du_in.at[:, parts[1]], du_v.at[:, parts[1]], lsem.at[2]),
             cp(n_in.at[:, pl.ds(DF, (steps - 1) * DF)], n_v.at[:, pl.ds(DF, (steps - 1) * DF)], lsem.at[3])]
    through = ((u_in, u_v, u_out), (x_in, x_v, x_out), (de_in, de_v, de_out), (dg_in, dg_v, dg_out))
    ins = [cp(a, b, psem.at[k]) for k, (a, b, _) in enumerate(through)]
    outs = [cp(b, c, qsem.at[k]) for k, (_, b, c) in enumerate(through)]
    for c in loads + ins:
        c.start()

    def store(i, slot):
        return cp(ring.at[slot], dw_out.at[pl.ds(pl.multiple_of(i * DF, DF), DF)], osem.at[slot])

    loads[0].wait()
    loads[1].wait()

    def step(i, carry):
        slot = lax.rem(i, RS)
        sl = pl.ds(pl.multiple_of(i * DF, DF), DF)

        @pl.when(i >= RS)
        def _():
            store(i - RS, slot).wait()

        @pl.when(i == 1)
        def _():
            loads[3].wait()

        for k, part in enumerate(parts):
            if k == 1:
                @pl.when(i == 0)
                def _():
                    loads[2].wait()
            ring[slot, :, part] = lax.dot_general(n_v[:, sl], du_v[:, part], (((0,), (0,)), ((), ())),
                                                  preferred_element_type=F32)
        store(i, slot).start()

        @pl.when(i == 2)
        def _():
            for a, b in zip(ins, outs):
                a.wait()
                b.start()

        return carry

    lax.fori_loop(0, steps, step, 0)
    for i in range(steps - RS, steps):
        store(i, i % RS).wait()
    for c in outs:
        c.wait()


def solution(mesh):
    group_size = mesh.shape['tp']

    def local_step(token_ids, table_loc, gain_vec, w_loc, du_loc, dres_loc):
        num_micro, seq_len = token_ids.shape
        rows_loc, model_dim = table_loc.shape
        seq_loc = seq_len // group_size
        cols_loc = w_loc.shape[1]
        tokens = num_micro * seq_len
        du_flat = du_loc.reshape(tokens, cols_loc)
        vm, hb = pl.BlockSpec(memory_space=pltpu.VMEM), pl.BlockSpec(memory_space=pl.ANY)
        sd = jax.ShapeDtypeStruct
        dma = pltpu.SemaphoreType.DMA
        u_all, x_own, normed, grad_table, grad_gain = pl.pallas_call(
            _k1,
            out_shape=(sd((tokens, cols_loc), BF16), sd((num_micro, seq_loc, model_dim), BF16),
                       sd((tokens, model_dim), BF16), sd((rows_loc, model_dim), F32), sd((1, model_dim), F32)),
            in_specs=[vm, vm, hb, hb, hb, hb],
            out_specs=(hb, hb, hb, vm, vm),
            scratch_shapes=[
                pltpu.VMEM((tokens, cols_loc), BF16),
                pltpu.VMEM((WS, FB, cols_loc), BF16),
                pltpu.VMEM((8, 64, model_dim), BF16),
                pltpu.VMEM((NB, 2, 2, 2, 2, 32, FB), BF16),
                pltpu.VMEM((NB, 2, 3, 2, 32, FB), BF16),
                pltpu.VMEM((2, NB, 32, FB), F32),
                pltpu.VMEM((2, NB, 32, FB), F32),
                pltpu.VMEM((2, NB, 32, FB), F32),
                pltpu.VMEM((CS, model_dim, UC), BF16),
                pltpu.VMEM((2, tokens, UC), BF16),
                pltpu.VMEM((tokens, model_dim), BF16),
                pltpu.VMEM((64, model_dim), F32),
                pltpu.VMEM((64, 128), F32),
                pltpu.VMEM((2, 32, model_dim), BF16),
                pltpu.VMEM((2, 32, model_dim), BF16),
                pltpu.VMEM((2, 8, 32, model_dim), BF16),
                pltpu.VMEM((8, 1, model_dim), F32),
                dma((4,)), dma((WS,)), dma((CS,)), dma((2,)),
                dma((16,)), dma((16,)),
                dma((NB, 2, 3)), dma((NB, 2, 3)), dma((2, NB)), dma((2, NB)),
                dma((2, 14)), dma((2, 16)),
                dma((8,)), dma((8,)),
            ],
            compiler_params=pltpu.CompilerParams(collective_id=0, has_side_effects=True,
                                                 vmem_limit_bytes=67043328),
            name="k1",
        )(token_ids, gain_vec, table_loc, w_loc,
          du_flat, dres_loc)
        grad_w, u_all, x_own, grad_table, grad_gain = pl.pallas_call(
            _k2,
            out_shape=(sd((model_dim, cols_loc), F32), sd((tokens, cols_loc), BF16),
                       sd((num_micro, seq_loc, model_dim), BF16), sd((rows_loc, model_dim), F32),
                       sd((1, model_dim), F32)),
            in_specs=[hb] * 6,
            out_specs=(hb,) * 5,
            scratch_shapes=[
                pltpu.VMEM((tokens, model_dim), BF16), pltpu.VMEM((tokens, cols_loc), BF16),
                pltpu.VMEM((RS, DF, cols_loc), F32),
                pltpu.VMEM((tokens, cols_loc), BF16), pltpu.VMEM((num_micro, seq_loc, model_dim), BF16),
                pltpu.VMEM((rows_loc, model_dim), F32), pltpu.VMEM((1, model_dim), F32),
                dma((4,)), dma((4,)), dma((4,)), dma((RS,)),
            ],
            compiler_params=pltpu.CompilerParams(vmem_limit_bytes=60 * 2 ** 20),
            name="k2",
        )(normed, du_flat, u_all, x_own, grad_table, grad_gain)
        return u_all.reshape(num_micro, seq_len, cols_loc), x_own, grad_table, grad_w, grad_gain.reshape(model_dim)

    return jax.shard_map(local_step, mesh=mesh,
                         in_specs=(P('dp', None), P('tp', None), P(None), P(None, 'tp'), P('dp', None, 'tp'), P('dp', 'tp', None)),
                         out_specs=(P('dp', None, 'tp'), P('dp', 'tp', None), P(('dp', 'tp'), None), P(None, ('dp', 'tp')), P('dp')),
                         check_vma=False)
```

```python
import functools

import jax
import jax.numpy as jnp
from jax import lax
from jax.experimental import pallas as pl
from jax.experimental.pallas import tpu as pltpu
from jax.sharding import PartitionSpec as P

NORM_EPS = 1e-6
MESH = pl.DeviceIdType.MESH
F32 = jnp.float32
BF16 = jnp.bfloat16
FB = 512
NB = 8
UC = 256
TB = 128
DF = 256
RS = 4
WS = 3
CS = 4


def _flip(r, bits):
    for bit in (1, 2, 4):
        if bits & bit:
            r = r + bit - 2 * bit * (lax.rem(lax.div(r, bit), 2))
    return r


def _rcopy(src, dst, ssem, rsem, dev, dp=None):
    return pltpu.make_async_remote_copy(src_ref=src, dst_ref=dst, send_sem=ssem, recv_sem=rsem,
                                        device_id={"tp": dev} if dp is None else {"dp": dp, "tp": dev},
                                        device_id_type=MESH)


class _Gather:
    def __init__(self, r, chunk, ssem, rsem):
        self.r, self.chunk, self.ssem, self.rsem = r, chunk, ssem, rsem

    def send(self, rel_owner, h, to, idx):
        owner = _flip(self.r, rel_owner)
        return _rcopy(self.chunk(owner, h), self.chunk(owner, h), self.ssem.at[idx], self.rsem.at[2 * (rel_owner ^ to) + h],
                      _flip(self.r, to))

    def wait_in(self, rel_owner, h):
        owner = _flip(self.r, rel_owner)
        _rcopy(self.chunk(owner, h), self.chunk(owner, h), self.ssem.at[0], self.rsem.at[2 * rel_owner + h],
               _flip(self.r, 1)).wait_recv()

    def own(self):
        self.send(0, 0, 2, 0).start()
        self.send(0, 1, 4, 1).start()
        self.send(0, 1, 2, 2).start()
        self.send(0, 0, 4, 3).start()
        self.send(0, 0, 1, 4).start()
        self.send(0, 1, 1, 5).start()

    def fwd1(self):
        self.wait_in(2, 0)
        self.send(2, 0, 4, 6).start()
        self.send(2, 0, 1, 7).start()
        self.wait_in(4, 1)
        self.send(4, 1, 2, 8).start()
        self.send(4, 1, 1, 9).start()

    def fwd2(self):
        self.wait_in(2, 1)
        self.send(2, 1, 1, 10).start()
        self.wait_in(4, 0)
        self.send(4, 0, 1, 11).start()

    def fwd3(self):
        self.wait_in(6, 0)
        self.send(6, 0, 1, 12).start()
        self.wait_in(6, 1)
        self.send(6, 1, 1, 13).start()

    def finish(self):
        for rel in (1, 3, 5, 7):
            for h in (0, 1):
                self.wait_in(rel, h)
        for idx in range(14):
            self.send(0, 0, 1, idx).wait_send()


class _TableGather:
    def __init__(self, r, p, buf, tab, ssem, rsem):
        self.r, self.p, self.buf, self.tab, self.ssem, self.rsem = r, p, buf, tab, ssem, rsem

    def rows(self, k):
        return pl.ds(pl.multiple_of(16 * (k + self.p * (3 - 2 * k)), 16), 16)

    def own(self):
        for n, (to, k) in enumerate(((2, 0), (4, 2), (2, 1), (4, 3))):
            _rcopy(self.tab.at[self.rows(k)], self.buf.at[self.r, self.rows(k)], self.ssem.at[n],
                   self.rsem.at[2 * to + k], _flip(self.r, to)).start()
        _rcopy(self.tab, self.buf.at[self.r], self.ssem.at[4], self.rsem.at[0], _flip(self.r, 1)).start()

    def wait_in(self, rel, k):
        src = self.buf.at[_flip(self.r, rel), self.rows(k)]
        _rcopy(src, src, self.ssem.at[0], self.rsem.at[2 * rel + k], _flip(self.r, 1)).wait_recv()

    def fwd(self, rel, k, to, idx):
        src = self.buf.at[_flip(self.r, rel), self.rows(k)]
        _rcopy(src, src, self.ssem.at[idx], self.rsem.at[2 * (rel ^ to) + k], _flip(self.r, to)).start()

    def twin(self, rel, k, idx):
        src = self.buf.at[_flip(self.r, rel), self.rows(k)]
        _rcopy(src, src, self.ssem.at[idx], self.rsem.at[2 * rel + 3 - k], self.r, 1 - self.p).start()

    def block(self, rel, idx, start):
        src = self.buf.at[_flip(self.r, rel)]
        c = _rcopy(src, src, self.ssem.at[idx], self.rsem.at[rel // 2], _flip(self.r, 1))
        if start:
            c.start()
        else:
            c.wait_recv()

    def relay(self, n):
        for rel, k, to in ((2, n, 4), (4, 2 + n, 2)):
            self.wait_in(rel, k)
            self.fwd(rel, k, to, 5 + 2 * n + (rel // 4))
            self.twin(rel, k, 9 + 2 * n + (rel // 4))

    def blocks(self):
        for n, (rel, ks) in enumerate(((2, (2, 3)), (4, (0, 1)), (6, (0, 1, 2, 3)))):
            for k in ks:
                self.wait_in(rel, k)
            self.block(rel, 13 + n, True)

    def finish(self):
        _rcopy(self.tab, self.buf.at[self.r], self.ssem.at[4], self.rsem.at[0], _flip(self.r, 1)).wait_recv()
        for n, rel in enumerate((2, 4, 6)):
            self.block(rel, 13 + n, False)
        small = self.buf.at[self.r, self.rows(0)]
        for n in range(16):
            src = self.buf.at[self.r] if n in (4, 13, 14, 15) else small
            _rcopy(src, src, self.ssem.at[n], self.rsem.at[0], _flip(self.r, 1)).wait_send()


def _k1(ids, gain, tab, w, du, dres, u_out, x_out, n_out, de_out, dg_out,
        du_v, w_v, etab, dn_v, rx1, tx2, rx2, own, wc_v, u_v, n_v, nh_v, inv_v, x_v, dres_v, dx_all, dgs,
        lsem, wsem, wcsem, usem, e_s, e_r, s1, r1, s2, r2, a_s, a_r, g_s, g_r):
    r = lax.axis_index("tp")
    p = lax.axis_index("dp")
    core = lax.rem(r, 2)
    xs = lax.rem(lax.div(r, 2), 2)
    ys = lax.div(r, 4)
    cols = w.shape[1]
    n_u = cols // UC

    du_cp = pltpu.make_async_copy(du, du_v, lsem.at[0])
    du_cp.start()

    def w_cp(j, slot):
        return pltpu.make_async_copy(w.at[pl.ds(pl.multiple_of(j * FB, FB), FB)], w_v.at[slot], wsem.at[slot])

    def wc_cp(i, slot):
        return pltpu.make_async_copy(w.at[:, pl.ds(pl.multiple_of(i * UC, UC), UC)], wc_v.at[slot], wcsem.at[slot])

    def u_cp(i, slot):
        return pltpu.make_async_copy(u_v.at[slot], u_out.at[:, pl.ds(pl.multiple_of(i * UC, UC), UC)], usem.at[slot])

    for k in range(WS - 1):
        w_cp(k, k).start()
    tab_cp = pltpu.make_async_copy(tab, etab.at[r], lsem.at[2])
    tab_cp.start()
    dres_cp = pltpu.make_async_copy(dres, dres_v, lsem.at[3])
    dres_cp.start()

    barrier = pltpu.get_barrier_semaphore()
    for rel in range(1, 8):
        pl.semaphore_signal(barrier, inc=1, device_id={"tp": _flip(r, rel)}, device_id_type=MESH)
    pl.semaphore_signal(barrier, inc=1, device_id={"dp": 1 - p, "tp": r}, device_id_type=MESH)
    pl.semaphore_wait(barrier, 8)

    eg = _TableGather(r, p, etab, tab, e_s, e_r)
    eg.own()
    du_cp.wait()

    def rs1(j, m, even):
        if even:
            sib = dn_v.at[j, m, :, xs, 1 - core]
            far = [dn_v.at[j, m, :, 1 - xs, c] for c in range(2)]
            dev = [(ys * 2 + 1 - xs) * 2 + c for c in range(2)]
        else:
            sib = dn_v.at[j, m, ys, :, 1 - core]
            far = [dn_v.at[j, m, 1 - ys, :, c] for c in range(2)]
            dev = [((1 - ys) * 2 + xs) * 2 + c for c in range(2)]
        out = [_rcopy(far[c], rx1.at[j, m, 1 + core], s1.at[j, m, 1 + c], r1.at[j, m, 1 + core], dev[c])
               for c in range(2)]
        out.append(_rcopy(sib, rx1.at[j, m, 0], s1.at[j, m, 0], r1.at[j, m, 0], _flip(r, 1)))
        return out

    def rs1_start(j, m):
        if isinstance(j, int):
            for c in rs1(j, m, j % 2 == 0):
                c.start()
            return

        @pl.when(lax.rem(j, 2) == 0)
        def _():
            for c in rs1(j, m, True):
                c.start()

        @pl.when(lax.rem(j, 2) == 1)
        def _():
            for c in rs1(j, m, False):
                c.start()

    def combine(m, pair):
        for j in (2 * pair, 2 * pair + 1):
            oy, ox, q = (1 - ys, xs, ys) if j % 2 == 0 else (ys, 1 - xs, xs)
            for n in range(3):
                _rcopy(rx1.at[j, m, n], rx1.at[j, m, n], s1.at[j, m, 0], r1.at[j, m, n], _flip(r, 1)).wait_recv()

            def total(part, qi):
                t = part.astype(F32)
                for n in range(3):
                    t = t + rx1[j, m, n, qi].astype(F32)
                return t

            tx2[m, j] = total(dn_v[j, m, oy, ox, core], 1 - q)
            own[m, j] = total(dn_v[j, m, ys, xs, core], q)

    def rs2(m, j):
        oy, ox = (1 - ys, xs) if j % 2 == 0 else (ys, 1 - xs)
        return _rcopy(tx2.at[m, j], rx2.at[m, j], s2.at[m, j], r2.at[m, j], (oy * 2 + ox) * 2 + core)

    def rs2_start(m, pair):
        rs2(m, 2 * pair).start()
        rs2(m, 2 * pair + 1).start()

    def dn_step(j, carry):
        slot = lax.rem(j, WS)
        w_cp(j, slot).wait()

        @pl.when(j + WS - 1 < NB)
        def _():
            w_cp(j + WS - 1, lax.rem(j + WS - 1, WS)).start()

        part = lax.dot_general(du_v[...], w_v[slot], (((1,), (1,)), ((), ())),
                               preferred_element_type=F32)
        dn_v[j] = part.astype(BF16).reshape(2, 2, 2, 2, 32, FB)

        for n in range(2):
            @pl.when(j == n)
            def _():
                eg.relay(n)

        @pl.when(j == 2)
        def _():
            rs1_start(0, 0)

        @pl.when(j > 1)
        def _():
            rs1_start(j - 1, 0)

        @pl.when(j > 3)
        def _():
            rs1_start(j - 4, 1)

        @pl.when(j == 5)
        def _():
            eg.blocks()

        @pl.when(j == 6)
        def _():
            combine(0, 0)

        @pl.when(j == 7)
        def _():
            rs2_start(0, 0)
            combine(0, 1)

        @pl.when(j == NB - 2)
        def _():
            for k in range(CS - 1):
                wc_cp(k, k).start()

        return carry

    lax.fori_loop(0, NB, dn_step, 0)
    tab_cp.wait()
    rs1_start(7, 0)
    rs2_start(0, 1)
    rs1_start(4, 1)
    rs1_start(5, 1)
    eg.finish()

    gf = gain[...].astype(F32).reshape(1, 4096)

    def one_hot(first, rows, tok):
        return (tok == first + lax.broadcasted_iota(jnp.int32, (rows, tok.shape[1]), 0)).astype(BF16)

    def lookup(pick_t):
        return lax.dot_general(pick_t, etab[...].reshape(512, 4096), (((0,), (0,)), ((), ())),
                               preferred_element_type=F32)

    for b in range(512 // TB):
        rows = slice(b * TB, (b + 1) * TB)
        col = b * TB % 256
        xg = lookup(one_hot(0, 512, ids[b * TB // 256:b * TB // 256 + 1, col:col + TB]))
        inv = lax.rsqrt(jnp.mean(xg * xg, axis=-1, keepdims=True) + NORM_EPS)
        n_v[rows, :] = (xg * inv * gf).astype(BF16)

    n_cp = pltpu.make_async_copy(n_v, n_out, lsem.at[0])
    n_cp.start()

    mine = (lax.broadcasted_iota(jnp.int32, (32, 256), 1) ==
            r * 32 + lax.broadcasted_iota(jnp.int32, (32, 256), 0)).astype(BF16)
    pick_own = jnp.concatenate(
        [lax.dot_general(mine, one_hot(0, 512, ids[m:m + 1, :]), (((1,), (1,)), ((), ())), preferred_element_type=F32)
         for m in range(2)], axis=0).astype(BF16)
    xo = jnp.dot(pick_own, etab[...].reshape(512, 4096), preferred_element_type=F32)
    inv_own = lax.rsqrt(jnp.mean(xo * xo, axis=-1, keepdims=True) + NORM_EPS)
    x_v[...] = xo.astype(BF16).reshape(2, 32, 4096)
    nh_v[...] = xo * inv_own
    inv_v[...] = jnp.broadcast_to(inv_own, (64, 128))
    x_cp = pltpu.make_async_copy(x_v, x_out, lsem.at[1])
    x_cp.start()

    def dx_of(m):
        rows = slice(32 * m, 32 * m + 32)
        centre = jnp.zeros((32, 1), F32)
        for j in range(NB):
            sl = slice(j * FB, (j + 1) * FB)
            rs2(m, j).wait_recv()
            dn = own[m, j] + rx2[m, j]
            own[m, j] = dn
            nh = nh_v[rows, sl]
            centre = centre + jnp.sum(nh * (gf[:, sl] * dn), axis=-1, keepdims=True)
            part = jnp.sum(dn * nh, axis=0, keepdims=True)
            dgs[r, :, sl] = part if m == 0 else dgs[r, :, sl] + part
        centre = centre * (1.0 / 4096)
        for j in range(NB):
            sl = slice(j * FB, (j + 1) * FB)
            dr = dres_v[m, :, sl].astype(F32)
            dx = dr + inv_v[rows, 0:1] * (gf[:, sl] * own[m, j] - nh_v[rows, sl] * centre)
            dx_all[m, r, :, sl] = dx.astype(BF16)

    def dx_gather(m):
        return _Gather(r, lambda owner, h: dx_all.at[m, owner, pl.ds(16 * h, 16)], a_s.at[m], a_r.at[m])

    ag = [dx_gather(m) for m in range(2)]
    dres_cp.wait()
    events = {
        0: lambda: (combine(0, 2),),
        1: lambda: (rs2_start(0, 2), combine(0, 3),),
        2: lambda: (rs2_start(0, 3), rs1_start(6, 1), rs1_start(7, 1), combine(1, 0),),
        3: lambda: (rs2_start(1, 0), combine(1, 1),),
        4: lambda: (rs2_start(1, 1), combine(1, 2),),
        5: lambda: (rs2_start(1, 2), dx_of(0),),
        6: lambda: (combine(1, 3),),
        7: lambda: (rs2_start(1, 3), ag[0].own(),),
        9: lambda: (dx_of(1),),
        10: lambda: (ag[1].own(),),
        11: lambda: (ag[0].fwd1(),),
        13: lambda: (ag[0].fwd2(),),
        15: lambda: (ag[1].fwd1(),),
    }

    def u_step(i, carry):
        slot = lax.rem(i, 2)
        wslot = lax.rem(i, CS)
        wc_cp(i, wslot).wait()

        @pl.when(i + CS - 1 < n_u)
        def _():
            wc_cp(i + CS - 1, lax.rem(i + CS - 1, CS)).start()

        @pl.when(i >= 2)
        def _():
            u_cp(i - 2, slot).wait()

        u_v[slot] = jnp.dot(n_v[...], wc_v[wslot], preferred_element_type=F32).astype(BF16)
        u_cp(i, slot).start()

        for at, event in events.items():
            pl.when(i == at)(lambda event=event: (event(), None)[1])

        return carry

    lax.fori_loop(0, n_u, u_step, 0)
    def dg_cp(rel):
        return _rcopy(dgs.at[r], dgs.at[r], g_s.at[rel], g_r.at[r], _flip(r, rel))

    for rel in range(1, 8):
        dg_cp(rel).start()
    ag[0].fwd3()
    u_cp(n_u - 2, n_u % 2).wait()
    u_cp(n_u - 1, (n_u - 1) % 2).wait()
    ag[0].finish()
    ag[1].fwd2()

    def grad_rows(m):
        return jnp.dot(one_hot(r * 64, 64, ids[m:m + 1, :]), dx_all[m].reshape(256, 4096), preferred_element_type=F32)

    de = grad_rows(0)
    ag[1].fwd3()
    for rel in range(1, 8):
        src = _flip(r, rel)
        _rcopy(dgs.at[src], dgs.at[src], g_s.at[rel], g_r.at[src], src).wait_recv()
    tot = dgs[0]
    for k in range(1, 8):
        tot = tot + dgs[k]
    dg_out[...] = tot
    ag[1].finish()
    de_out[...] = de + grad_rows(1)

    for rel in range(1, 8):
        dg_cp(rel).wait_send()
    for m in range(2):
        for j in range(NB):
            for c in rs1(j, m, j % 2 == 0):
                c.wait_send()
            rs2(m, j).wait_send()
    n_cp.wait()
    x_cp.wait()


def _k2(n_in, du_in, u_in, x_in, de_in, dg_in, dw_out, u_out, x_out, de_out, dg_out,
        n_v, du_v, ring, u_v, x_v, de_v, dg_v, lsem, psem, qsem, osem):
    steps = n_in.shape[1] // DF
    half = 9 * 256
    cols = du_in.shape[1]
    parts = (pl.ds(0, half), pl.ds(half, cols - half))
    cp = pltpu.make_async_copy
    loads = [cp(n_in.at[:, pl.ds(0, DF)], n_v.at[:, pl.ds(0, DF)], lsem.at[0]),
             cp(du_in.at[:, parts[0]], du_v.at[:, parts[0]], lsem.at[1]),
             cp(du_in.at[:, parts[1]], du_v.at[:, parts[1]], lsem.at[2]),
             cp(n_in.at[:, pl.ds(DF, (steps - 1) * DF)], n_v.at[:, pl.ds(DF, (steps - 1) * DF)], lsem.at[3])]
    through = ((u_in, u_v, u_out), (x_in, x_v, x_out), (de_in, de_v, de_out), (dg_in, dg_v, dg_out))
    ins = [cp(a, b, psem.at[k]) for k, (a, b, _) in enumerate(through)]
    outs = [cp(b, c, qsem.at[k]) for k, (_, b, c) in enumerate(through)]
    for c in loads + ins:
        c.start()

    def store(i, slot):
        return cp(ring.at[slot], dw_out.at[pl.ds(pl.multiple_of(i * DF, DF), DF)], osem.at[slot])

    loads[0].wait()
    loads[1].wait()

    def step(i, carry):
        slot = lax.rem(i, RS)
        sl = pl.ds(pl.multiple_of(i * DF, DF), DF)

        @pl.when(i >= RS)
        def _():
            store(i - RS, slot).wait()

        @pl.when(i == 1)
        def _():
            loads[3].wait()

        for k, part in enumerate(parts):
            if k == 1:
                @pl.when(i == 0)
                def _():
                    loads[2].wait()
            ring[slot, :, part] = lax.dot_general(n_v[:, sl], du_v[:, part], (((0,), (0,)), ((), ())),
                                                  preferred_element_type=F32)
        store(i, slot).start()

        @pl.when(i == 2)
        def _():
            for a, b in zip(ins, outs):
                a.wait()
                b.start()

        return carry

    lax.fori_loop(0, steps, step, 0)
    for i in range(steps - RS, steps):
        store(i, i % RS).wait()
    for c in outs:
        c.wait()


def solution(mesh):
    group_size = mesh.shape['tp']

    def local_step(token_ids, table_loc, gain_vec, w_loc, du_loc, dres_loc):
        num_micro, seq_len = token_ids.shape
        rows_loc, model_dim = table_loc.shape
        seq_loc = seq_len // group_size
        cols_loc = w_loc.shape[1]
        tokens = num_micro * seq_len
        du_flat = du_loc.reshape(tokens, cols_loc)
        vm, hb = pl.BlockSpec(memory_space=pltpu.VMEM), pl.BlockSpec(memory_space=pl.ANY)
        sd = jax.ShapeDtypeStruct
        dma = pltpu.SemaphoreType.DMA
        u_all, x_own, normed, grad_table, grad_gain = pl.pallas_call(
            _k1,
            out_shape=(sd((tokens, cols_loc), BF16), sd((num_micro, seq_loc, model_dim), BF16),
                       sd((tokens, model_dim), BF16), sd((rows_loc, model_dim), F32), sd((1, model_dim), F32)),
            in_specs=[vm, vm, hb, hb, hb, hb],
            out_specs=(hb, hb, hb, vm, vm),
            scratch_shapes=[
                pltpu.VMEM((tokens, cols_loc), BF16),
                pltpu.VMEM((WS, FB, cols_loc), BF16),
                pltpu.VMEM((8, 64, model_dim), BF16),
                pltpu.VMEM((NB, 2, 2, 2, 2, 32, FB), BF16),
                pltpu.VMEM((NB, 2, 3, 2, 32, FB), BF16),
                pltpu.VMEM((2, NB, 32, FB), F32),
                pltpu.VMEM((2, NB, 32, FB), F32),
                pltpu.VMEM((2, NB, 32, FB), F32),
                pltpu.VMEM((CS, model_dim, UC), BF16),
                pltpu.VMEM((2, tokens, UC), BF16),
                pltpu.VMEM((tokens, model_dim), BF16),
                pltpu.VMEM((64, model_dim), F32),
                pltpu.VMEM((64, 128), F32),
                pltpu.VMEM((2, 32, model_dim), BF16),
                pltpu.VMEM((2, 32, model_dim), BF16),
                pltpu.VMEM((2, 8, 32, model_dim), BF16),
                pltpu.VMEM((8, 1, model_dim), F32),
                dma((4,)), dma((WS,)), dma((CS,)), dma((2,)),
                dma((16,)), dma((16,)),
                dma((NB, 2, 3)), dma((NB, 2, 3)), dma((2, NB)), dma((2, NB)),
                dma((2, 14)), dma((2, 16)),
                dma((8,)), dma((8,)),
            ],
            compiler_params=pltpu.CompilerParams(collective_id=0, has_side_effects=True,
                                                 vmem_limit_bytes=67043328),
            name="k1",
        )(token_ids, gain_vec, table_loc, w_loc,
          du_flat, dres_loc)
        grad_w, u_all, x_own, grad_table, grad_gain = pl.pallas_call(
            _k2,
            out_shape=(sd((model_dim, cols_loc), F32), sd((tokens, cols_loc), BF16),
                       sd((num_micro, seq_loc, model_dim), BF16), sd((rows_loc, model_dim), F32),
                       sd((1, model_dim), F32)),
            in_specs=[hb] * 6,
            out_specs=(hb,) * 5,
            scratch_shapes=[
                pltpu.VMEM((tokens, model_dim), BF16), pltpu.VMEM((tokens, cols_loc), BF16),
                pltpu.VMEM((RS, DF, cols_loc), F32),
                pltpu.VMEM((tokens, cols_loc), BF16), pltpu.VMEM((num_micro, seq_loc, model_dim), BF16),
                pltpu.VMEM((rows_loc, model_dim), F32), pltpu.VMEM((1, model_dim), F32),
                dma((4,)), dma((4,)), dma((4,)), dma((RS,)),
            ],
            compiler_params=pltpu.CompilerParams(vmem_limit_bytes=60 * 2 ** 20),
            name="k2",
        )(normed, du_flat, u_all, x_own, grad_table, grad_gain)
        return u_all.reshape(num_micro, seq_len, cols_loc), x_own, grad_table, grad_w, grad_gain.reshape(model_dim)

    return jax.shard_map(local_step, mesh=mesh,
                         in_specs=(P('dp', None), P('tp', None), P(None), P(None, 'tp'), P('dp', None, 'tp'), P('dp', 'tp', None)),
                         out_specs=(P('dp', None, 'tp'), P('dp', 'tp', None), P(('dp', 'tp'), None), P(None, ('dp', 'tp')), P('dp')),
                         check_vma=False)
```

```python
import functools

import jax
import jax.numpy as jnp
from jax import lax
from jax.experimental import pallas as pl
from jax.experimental.pallas import tpu as pltpu
from jax.sharding import PartitionSpec as P

NORM_EPS = 1e-6
MESH = pl.DeviceIdType.MESH
F32 = jnp.float32
BF16 = jnp.bfloat16
FB = 512
NB = 8
UC = 256
TB = 128
DF = 256
RS = 4
WS = 3
CS = 4


def _flip(r, bits):
    for bit in (1, 2, 4):
        if bits & bit:
            r = r + bit - 2 * bit * (lax.rem(lax.div(r, bit), 2))
    return r


def _rcopy(src, dst, ssem, rsem, dev, dp=None):
    return pltpu.make_async_remote_copy(src_ref=src, dst_ref=dst, send_sem=ssem, recv_sem=rsem,
                                        device_id={"tp": dev} if dp is None else {"dp": dp, "tp": dev},
                                        device_id_type=MESH)


class _Gather:
    def __init__(self, r, chunk, ssem, rsem):
        self.r, self.chunk, self.ssem, self.rsem = r, chunk, ssem, rsem

    def send(self, rel_owner, h, to, idx):
        owner = _flip(self.r, rel_owner)
        return _rcopy(self.chunk(owner, h), self.chunk(owner, h), self.ssem.at[idx], self.rsem.at[2 * (rel_owner ^ to) + h],
                      _flip(self.r, to))

    def wait_in(self, rel_owner, h):
        owner = _flip(self.r, rel_owner)
        _rcopy(self.chunk(owner, h), self.chunk(owner, h), self.ssem.at[0], self.rsem.at[2 * rel_owner + h],
               _flip(self.r, 1)).wait_recv()

    def own(self):
        self.send(0, 0, 2, 0).start()
        self.send(0, 1, 4, 1).start()
        self.send(0, 1, 2, 2).start()
        self.send(0, 0, 4, 3).start()
        self.send(0, 0, 1, 4).start()
        self.send(0, 1, 1, 5).start()

    def fwd1(self):
        self.wait_in(2, 0)
        self.send(2, 0, 4, 6).start()
        self.send(2, 0, 1, 7).start()
        self.wait_in(4, 1)
        self.send(4, 1, 2, 8).start()
        self.send(4, 1, 1, 9).start()

    def fwd2(self):
        self.wait_in(2, 1)
        self.send(2, 1, 1, 10).start()
        self.wait_in(4, 0)
        self.send(4, 0, 1, 11).start()

    def fwd3(self):
        self.wait_in(6, 0)
        self.send(6, 0, 1, 12).start()
        self.wait_in(6, 1)
        self.send(6, 1, 1, 13).start()

    def finish(self):
        for rel in (1, 3, 5, 7):
            for h in (0, 1):
                self.wait_in(rel, h)
        for idx in range(14):
            self.send(0, 0, 1, idx).wait_send()


class _TableGather:
    def __init__(self, r, p, buf, tab, ssem, rsem):
        self.r, self.p, self.buf, self.tab, self.ssem, self.rsem = r, p, buf, tab, ssem, rsem

    def rows(self, k):
        return pl.ds(pl.multiple_of(16 * (k + self.p * (3 - 2 * k)), 16), 16)

    def own(self):
        for n, (to, k) in enumerate(((2, 0), (4, 2), (2, 1), (4, 3))):
            _rcopy(self.tab.at[self.rows(k)], self.buf.at[self.r, self.rows(k)], self.ssem.at[n],
                   self.rsem.at[2 * to + k], _flip(self.r, to)).start()
        _rcopy(self.tab, self.buf.at[self.r], self.ssem.at[4], self.rsem.at[0], _flip(self.r, 1)).start()

    def wait_in(self, rel, k):
        src = self.buf.at[_flip(self.r, rel), self.rows(k)]
        _rcopy(src, src, self.ssem.at[0], self.rsem.at[2 * rel + k], _flip(self.r, 1)).wait_recv()

    def fwd(self, rel, k, to, idx):
        src = self.buf.at[_flip(self.r, rel), self.rows(k)]
        _rcopy(src, src, self.ssem.at[idx], self.rsem.at[2 * (rel ^ to) + k], _flip(self.r, to)).start()

    def twin(self, rel, k, idx):
        src = self.buf.at[_flip(self.r, rel), self.rows(k)]
        _rcopy(src, src, self.ssem.at[idx], self.rsem.at[2 * rel + 3 - k], self.r, 1 - self.p).start()

    def block(self, rel, idx, start):
        src = self.buf.at[_flip(self.r, rel)]
        c = _rcopy(src, src, self.ssem.at[idx], self.rsem.at[rel // 2], _flip(self.r, 1))
        if start:
            c.start()
        else:
            c.wait_recv()

    def relay(self, n):
        for rel, k, to in ((2, n, 4), (4, 2 + n, 2)):
            self.wait_in(rel, k)
            self.fwd(rel, k, to, 5 + 2 * n + (rel // 4))
            self.twin(rel, k, 9 + 2 * n + (rel // 4))

    def blocks(self):
        for n, (rel, ks) in enumerate(((2, (2, 3)), (4, (0, 1)), (6, (0, 1, 2, 3)))):
            for k in ks:
                self.wait_in(rel, k)
            self.block(rel, 13 + n, True)

    def finish(self):
        _rcopy(self.tab, self.buf.at[self.r], self.ssem.at[4], self.rsem.at[0], _flip(self.r, 1)).wait_recv()
        for n, rel in enumerate((2, 4, 6)):
            self.block(rel, 13 + n, False)
        small = self.buf.at[self.r, self.rows(0)]
        for n in range(16):
            src = self.buf.at[self.r] if n in (4, 13, 14, 15) else small
            _rcopy(src, src, self.ssem.at[n], self.rsem.at[0], _flip(self.r, 1)).wait_send()


def _k1(ids, gain, tab, w, du, dres, u_out, x_out, n_out, de_out, dg_out,
        du_v, w_v, etab, dn_v, rx1, tx2, rx2, own, wc_v, u_v, n_v, nh_v, inv_v, x_v, dres_v, dx_all, dgs,
        lsem, wsem, wcsem, usem, e_s, e_r, s1, r1, s2, r2, a_s, a_r, g_s, g_r):
    r = lax.axis_index("tp")
    p = lax.axis_index("dp")
    core = lax.rem(r, 2)
    xs = lax.rem(lax.div(r, 2), 2)
    ys = lax.div(r, 4)
    cols = w.shape[1]
    n_u = cols // UC

    du_cp = pltpu.make_async_copy(du, du_v, lsem.at[0])
    du_cp.start()

    def w_cp(j, slot):
        return pltpu.make_async_copy(w.at[pl.ds(pl.multiple_of(j * FB, FB), FB)], w_v.at[slot], wsem.at[slot])

    def wc_cp(i, slot):
        return pltpu.make_async_copy(w.at[:, pl.ds(pl.multiple_of(i * UC, UC), UC)], wc_v.at[slot], wcsem.at[slot])

    def u_cp(i, slot):
        return pltpu.make_async_copy(u_v.at[slot], u_out.at[:, pl.ds(pl.multiple_of(i * UC, UC), UC)], usem.at[slot])

    for k in range(WS - 1):
        w_cp(k, k).start()
    tab_cp = pltpu.make_async_copy(tab, etab.at[r], lsem.at[2])
    tab_cp.start()
    dres_cp = pltpu.make_async_copy(dres, dres_v, lsem.at[3])
    dres_cp.start()

    barrier = pltpu.get_barrier_semaphore()
    for rel in range(1, 8):
        pl.semaphore_signal(barrier, inc=1, device_id={"tp": _flip(r, rel)}, device_id_type=MESH)
    pl.semaphore_signal(barrier, inc=1, device_id={"dp": 1 - p, "tp": r}, device_id_type=MESH)
    pl.semaphore_wait(barrier, 8)

    eg = _TableGather(r, p, etab, tab, e_s, e_r)
    eg.own()
    du_cp.wait()

    def rs1(j, m, even):
        if even:
            sib = dn_v.at[j, m, :, xs, 1 - core]
            far = [dn_v.at[j, m, :, 1 - xs, c] for c in range(2)]
            dev = [(ys * 2 + 1 - xs) * 2 + c for c in range(2)]
        else:
            sib = dn_v.at[j, m, ys, :, 1 - core]
            far = [dn_v.at[j, m, 1 - ys, :, c] for c in range(2)]
            dev = [((1 - ys) * 2 + xs) * 2 + c for c in range(2)]
        out = [_rcopy(far[c], rx1.at[j, m, 1 + core], s1.at[j, m, 1 + c], r1.at[j, m, 1 + core], dev[c])
               for c in range(2)]
        out.append(_rcopy(sib, rx1.at[j, m, 0], s1.at[j, m, 0], r1.at[j, m, 0], _flip(r, 1)))
        return out

    def rs1_start(j, m):
        if isinstance(j, int):
            for c in rs1(j, m, j % 2 == 0):
                c.start()
            return

        @pl.when(lax.rem(j, 2) == 0)
        def _():
            for c in rs1(j, m, True):
                c.start()

        @pl.when(lax.rem(j, 2) == 1)
        def _():
            for c in rs1(j, m, False):
                c.start()

    def combine(m, pair):
        for j in (2 * pair, 2 * pair + 1):
            oy, ox, q = (1 - ys, xs, ys) if j % 2 == 0 else (ys, 1 - xs, xs)
            for n in range(3):
                _rcopy(rx1.at[j, m, n], rx1.at[j, m, n], s1.at[j, m, 0], r1.at[j, m, n], _flip(r, 1)).wait_recv()

            def total(part, qi):
                t = part.astype(F32)
                for n in range(3):
                    t = t + rx1[j, m, n, qi].astype(F32)
                return t

            tx2[m, j] = total(dn_v[j, m, oy, ox, core], 1 - q)
            own[m, j] = total(dn_v[j, m, ys, xs, core], q)

    def rs2(m, j):
        oy, ox = (1 - ys, xs) if j % 2 == 0 else (ys, 1 - xs)
        return _rcopy(tx2.at[m, j], rx2.at[m, j], s2.at[m, j], r2.at[m, j], (oy * 2 + ox) * 2 + core)

    def rs2_start(m, pair):
        rs2(m, 2 * pair).start()
        rs2(m, 2 * pair + 1).start()

    def dn_step(j, carry):
        slot = lax.rem(j, WS)
        w_cp(j, slot).wait()

        @pl.when(j + WS - 1 < NB)
        def _():
            w_cp(j + WS - 1, lax.rem(j + WS - 1, WS)).start()

        part = lax.dot_general(du_v[...], w_v[slot], (((1,), (1,)), ((), ())),
                               preferred_element_type=F32)
        dn_v[j] = part.astype(BF16).reshape(2, 2, 2, 2, 32, FB)

        for n in range(2):
            @pl.when(j == n)
            def _():
                eg.relay(n)

        @pl.when(j == 2)
        def _():
            rs1_start(0, 0)

        @pl.when(j > 1)
        def _():
            rs1_start(j - 1, 0)

        @pl.when(j > 3)
        def _():
            rs1_start(j - 4, 1)

        @pl.when(j == 5)
        def _():
            eg.blocks()

        @pl.when(j == 6)
        def _():
            combine(0, 0)

        @pl.when(j == 7)
        def _():
            rs2_start(0, 0)
            combine(0, 1)

        @pl.when(j == NB - 2)
        def _():
            for k in range(CS - 1):
                wc_cp(k, k).start()

        return carry

    lax.fori_loop(0, NB, dn_step, 0)
    tab_cp.wait()
    rs1_start(7, 0)
    rs2_start(0, 1)
    rs1_start(4, 1)
    rs1_start(5, 1)
    eg.finish()

    gf = gain[...].astype(F32).reshape(1, 4096)

    def one_hot(first, rows, tok):
        return (tok == first + lax.broadcasted_iota(jnp.int32, (rows, tok.shape[1]), 0)).astype(BF16)

    def lookup(pick_t):
        return lax.dot_general(pick_t, etab[...].reshape(512, 4096), (((0,), (0,)), ((), ())),
                               preferred_element_type=F32)

    for b in range(512 // TB):
        rows = slice(b * TB, (b + 1) * TB)
        col = b * TB % 256
        xg = lookup(one_hot(0, 512, ids[b * TB // 256:b * TB // 256 + 1, col:col + TB]))
        inv = lax.rsqrt(jnp.mean(xg * xg, axis=-1, keepdims=True) + NORM_EPS)
        n_v[rows, :] = (xg * inv * gf).astype(BF16)

    n_cp = pltpu.make_async_copy(n_v, n_out, lsem.at[0])
    n_cp.start()

    mine = (lax.broadcasted_iota(jnp.int32, (32, 256), 1) ==
            r * 32 + lax.broadcasted_iota(jnp.int32, (32, 256), 0)).astype(BF16)
    pick_own = jnp.concatenate(
        [lax.dot_general(mine, one_hot(0, 512, ids[m:m + 1, :]), (((1,), (1,)), ((), ())), preferred_element_type=F32)
         for m in range(2)], axis=0).astype(BF16)
    xo = jnp.dot(pick_own, etab[...].reshape(512, 4096), preferred_element_type=F32)
    inv_own = lax.rsqrt(jnp.mean(xo * xo, axis=-1, keepdims=True) + NORM_EPS)
    x_v[...] = xo.astype(BF16).reshape(2, 32, 4096)
    nh_v[...] = xo * inv_own
    inv_v[...] = jnp.broadcast_to(inv_own, (64, 128))
    x_cp = pltpu.make_async_copy(x_v, x_out, lsem.at[1])
    x_cp.start()

    def dx_of(m):
        rows = slice(32 * m, 32 * m + 32)
        centre = jnp.zeros((32, 1), F32)
        for j in range(NB):
            sl = slice(j * FB, (j + 1) * FB)
            rs2(m, j).wait_recv()
            dn = own[m, j] + rx2[m, j]
            own[m, j] = dn
            nh = nh_v[rows, sl]
            centre = centre + jnp.sum(nh * (gf[:, sl] * dn), axis=-1, keepdims=True)
            part = jnp.sum(dn * nh, axis=0, keepdims=True)
            dgs[r, :, sl] = part if m == 0 else dgs[r, :, sl] + part
        centre = centre * (1.0 / 4096)
        for j in range(NB):
            sl = slice(j * FB, (j + 1) * FB)
            dr = dres_v[m, :, sl].astype(F32)
            dx = dr + inv_v[rows, 0:1] * (gf[:, sl] * own[m, j] - nh_v[rows, sl] * centre)
            dx_all[m, r, :, sl] = dx.astype(BF16)

    def dx_gather(m):
        return _Gather(r, lambda owner, h: dx_all.at[m, owner, pl.ds(16 * h, 16)], a_s.at[m], a_r.at[m])

    ag = [dx_gather(m) for m in range(2)]
    dres_cp.wait()
    events = {
        0: lambda: (combine(0, 2),),
        1: lambda: (rs2_start(0, 2), combine(0, 3),),
        2: lambda: (rs2_start(0, 3), rs1_start(6, 1), rs1_start(7, 1), combine(1, 0),),
        3: lambda: (rs2_start(1, 0), combine(1, 1),),
        4: lambda: (rs2_start(1, 1), combine(1, 2),),
        5: lambda: (rs2_start(1, 2), dx_of(0),),
        6: lambda: (combine(1, 3),),
        7: lambda: (rs2_start(1, 3), ag[0].own(),),
        9: lambda: (dx_of(1),),
        10: lambda: (ag[1].own(),),
        11: lambda: (ag[0].fwd1(),),
        13: lambda: (ag[0].fwd2(),),
        15: lambda: (ag[1].fwd1(),),
    }

    def u_step(i, carry):
        slot = lax.rem(i, 2)
        wslot = lax.rem(i, CS)
        wc_cp(i, wslot).wait()

        @pl.when(i + CS - 1 < n_u)
        def _():
            wc_cp(i + CS - 1, lax.rem(i + CS - 1, CS)).start()

        @pl.when(i >= 2)
        def _():
            u_cp(i - 2, slot).wait()

        u_v[slot] = jnp.dot(n_v[...], wc_v[wslot], preferred_element_type=F32).astype(BF16)
        u_cp(i, slot).start()

        for at, event in events.items():
            pl.when(i == at)(lambda event=event: (event(), None)[1])

        return carry

    lax.fori_loop(0, n_u, u_step, 0)
    def dg_cp(rel):
        return _rcopy(dgs.at[r], dgs.at[r], g_s.at[rel], g_r.at[r], _flip(r, rel))

    for rel in range(1, 8):
        dg_cp(rel).start()
    ag[0].fwd3()
    u_cp(n_u - 2, n_u % 2).wait()
    u_cp(n_u - 1, (n_u - 1) % 2).wait()
    ag[0].finish()
    ag[1].fwd2()

    def grad_rows(m):
        return jnp.dot(one_hot(r * 64, 64, ids[m:m + 1, :]), dx_all[m].reshape(256, 4096), preferred_element_type=F32)

    de = grad_rows(0)
    ag[1].fwd3()
    for rel in range(1, 8):
        src = _flip(r, rel)
        _rcopy(dgs.at[src], dgs.at[src], g_s.at[rel], g_r.at[src], src).wait_recv()
    tot = dgs[0]
    for k in range(1, 8):
        tot = tot + dgs[k]
    dg_out[...] = tot
    ag[1].finish()
    de_out[...] = de + grad_rows(1)

    for rel in range(1, 8):
        dg_cp(rel).wait_send()
    for m in range(2):
        for j in range(NB):
            for c in rs1(j, m, j % 2 == 0):
                c.wait_send()
            rs2(m, j).wait_send()
    n_cp.wait()
    x_cp.wait()


def _k2(n_in, du_in, u_in, x_in, de_in, dg_in, dw_out, u_out, x_out, de_out, dg_out,
        n_v, du_v, ring, u_v, x_v, de_v, dg_v, lsem, psem, qsem, osem):
    steps = n_in.shape[1] // DF
    half = 9 * 256
    cols = du_in.shape[1]
    parts = (pl.ds(0, half), pl.ds(half, cols - half))
    cp = pltpu.make_async_copy
    loads = [cp(n_in.at[:, pl.ds(0, DF)], n_v.at[:, pl.ds(0, DF)], lsem.at[0]),
             cp(du_in.at[:, parts[0]], du_v.at[:, parts[0]], lsem.at[1]),
             cp(du_in.at[:, parts[1]], du_v.at[:, parts[1]], lsem.at[2]),
             cp(n_in.at[:, pl.ds(DF, (steps - 1) * DF)], n_v.at[:, pl.ds(DF, (steps - 1) * DF)], lsem.at[3])]
    through = ((u_in, u_v, u_out), (x_in, x_v, x_out), (de_in, de_v, de_out), (dg_in, dg_v, dg_out))
    ins = [cp(a, b, psem.at[k]) for k, (a, b, _) in enumerate(through)]
    outs = [cp(b, c, qsem.at[k]) for k, (_, b, c) in enumerate(through)]
    for c in loads + ins:
        c.start()

    def store(i, slot):
        return cp(ring.at[slot], dw_out.at[pl.ds(pl.multiple_of(i * DF, DF), DF)], osem.at[slot])

    loads[0].wait()
    loads[1].wait()

    def step(i, carry):
        slot = lax.rem(i, RS)
        sl = pl.ds(pl.multiple_of(i * DF, DF), DF)

        @pl.when(i >= RS)
        def _():
            store(i - RS, slot).wait()

        @pl.when(i == 1)
        def _():
            loads[3].wait()

        @pl.when(i == 0)
        def _():
            loads[2].wait()

        ring[slot] = lax.dot_general(n_v[:, sl], du_v[...], (((0,), (0,)), ((), ())), preferred_element_type=F32)
        store(i, slot).start()

        @pl.when(i == 2)
        def _():
            for a, b in zip(ins, outs):
                a.wait()
                b.start()

        return carry

    lax.fori_loop(0, steps, step, 0)
    for i in range(steps - RS, steps):
        store(i, i % RS).wait()
    for c in outs:
        c.wait()


def solution(mesh):
    group_size = mesh.shape['tp']

    def local_step(token_ids, table_loc, gain_vec, w_loc, du_loc, dres_loc):
        num_micro, seq_len = token_ids.shape
        rows_loc, model_dim = table_loc.shape
        seq_loc = seq_len // group_size
        cols_loc = w_loc.shape[1]
        tokens = num_micro * seq_len
        du_flat = du_loc.reshape(tokens, cols_loc)
        vm, hb = pl.BlockSpec(memory_space=pltpu.VMEM), pl.BlockSpec(memory_space=pl.ANY)
        sd = jax.ShapeDtypeStruct
        dma = pltpu.SemaphoreType.DMA
        u_all, x_own, normed, grad_table, grad_gain = pl.pallas_call(
            _k1,
            out_shape=(sd((tokens, cols_loc), BF16), sd((num_micro, seq_loc, model_dim), BF16),
                       sd((tokens, model_dim), BF16), sd((rows_loc, model_dim), F32), sd((1, model_dim), F32)),
            in_specs=[vm, vm, hb, hb, hb, hb],
            out_specs=(hb, hb, hb, vm, vm),
            scratch_shapes=[
                pltpu.VMEM((tokens, cols_loc), BF16),
                pltpu.VMEM((WS, FB, cols_loc), BF16),
                pltpu.VMEM((8, 64, model_dim), BF16),
                pltpu.VMEM((NB, 2, 2, 2, 2, 32, FB), BF16),
                pltpu.VMEM((NB, 2, 3, 2, 32, FB), BF16),
                pltpu.VMEM((2, NB, 32, FB), F32),
                pltpu.VMEM((2, NB, 32, FB), F32),
                pltpu.VMEM((2, NB, 32, FB), F32),
                pltpu.VMEM((CS, model_dim, UC), BF16),
                pltpu.VMEM((2, tokens, UC), BF16),
                pltpu.VMEM((tokens, model_dim), BF16),
                pltpu.VMEM((64, model_dim), F32),
                pltpu.VMEM((64, 128), F32),
                pltpu.VMEM((2, 32, model_dim), BF16),
                pltpu.VMEM((2, 32, model_dim), BF16),
                pltpu.VMEM((2, 8, 32, model_dim), BF16),
                pltpu.VMEM((8, 1, model_dim), F32),
                dma((4,)), dma((WS,)), dma((CS,)), dma((2,)),
                dma((16,)), dma((16,)),
                dma((NB, 2, 3)), dma((NB, 2, 3)), dma((2, NB)), dma((2, NB)),
                dma((2, 14)), dma((2, 16)),
                dma((8,)), dma((8,)),
            ],
            compiler_params=pltpu.CompilerParams(collective_id=0, has_side_effects=True,
                                                 vmem_limit_bytes=67043328),
            name="k1",
        )(token_ids, gain_vec, table_loc, w_loc,
          du_flat, dres_loc)
        grad_w, u_all, x_own, grad_table, grad_gain = pl.pallas_call(
            _k2,
            out_shape=(sd((model_dim, cols_loc), F32), sd((tokens, cols_loc), BF16),
                       sd((num_micro, seq_loc, model_dim), BF16), sd((rows_loc, model_dim), F32),
                       sd((1, model_dim), F32)),
            in_specs=[hb] * 6,
            out_specs=(hb,) * 5,
            scratch_shapes=[
                pltpu.VMEM((tokens, model_dim), BF16), pltpu.VMEM((tokens, cols_loc), BF16),
                pltpu.VMEM((RS, DF, cols_loc), F32),
                pltpu.VMEM((tokens, cols_loc), BF16), pltpu.VMEM((num_micro, seq_loc, model_dim), BF16),
                pltpu.VMEM((rows_loc, model_dim), F32), pltpu.VMEM((1, model_dim), F32),
                dma((4,)), dma((4,)), dma((4,)), dma((RS,)),
            ],
            compiler_params=pltpu.CompilerParams(vmem_limit_bytes=60 * 2 ** 20),
            name="k2",
        )(normed, du_flat, u_all, x_own, grad_table, grad_gain)
        return u_all.reshape(num_micro, seq_len, cols_loc), x_own, grad_table, grad_w, grad_gain.reshape(model_dim)

    return jax.shard_map(local_step, mesh=mesh,
                         in_specs=(P('dp', None), P('tp', None), P(None), P(None, 'tp'), P('dp', None, 'tp'), P('dp', 'tp', None)),
                         out_specs=(P('dp', None, 'tp'), P('dp', 'tp', None), P(('dp', 'tp'), None), P(None, ('dp', 'tp')), P('dp')),
                         check_vma=False)
```

```python
import functools

import jax
import jax.numpy as jnp
from jax import lax
from jax.experimental import pallas as pl
from jax.experimental.pallas import tpu as pltpu
from jax.sharding import PartitionSpec as P

NORM_EPS = 1e-6
MESH = pl.DeviceIdType.MESH
F32 = jnp.float32
BF16 = jnp.bfloat16
FB = 512
NB = 8
UC = 256
TB = 128
DF = 256
RS = 4
WS = 3
CS = 4


def _flip(r, bits):
    for bit in (1, 2, 4):
        if bits & bit:
            r = r + bit - 2 * bit * (lax.rem(lax.div(r, bit), 2))
    return r


def _rcopy(src, dst, ssem, rsem, dev, dp=None):
    return pltpu.make_async_remote_copy(src_ref=src, dst_ref=dst, send_sem=ssem, recv_sem=rsem,
                                        device_id={"tp": dev} if dp is None else {"dp": dp, "tp": dev},
                                        device_id_type=MESH)


class _Gather:
    def __init__(self, r, chunk, ssem, rsem):
        self.r, self.chunk, self.ssem, self.rsem = r, chunk, ssem, rsem

    def send(self, rel_owner, h, to, idx):
        owner = _flip(self.r, rel_owner)
        return _rcopy(self.chunk(owner, h), self.chunk(owner, h), self.ssem.at[idx], self.rsem.at[2 * (rel_owner ^ to) + h],
                      _flip(self.r, to))

    def wait_in(self, rel_owner, h):
        owner = _flip(self.r, rel_owner)
        _rcopy(self.chunk(owner, h), self.chunk(owner, h), self.ssem.at[0], self.rsem.at[2 * rel_owner + h],
               _flip(self.r, 1)).wait_recv()

    def own(self):
        self.send(0, 0, 2, 0).start()
        self.send(0, 1, 4, 1).start()
        self.send(0, 1, 2, 2).start()
        self.send(0, 0, 4, 3).start()
        self.send(0, 0, 1, 4).start()
        self.send(0, 1, 1, 5).start()

    def fwd1(self):
        self.wait_in(2, 0)
        self.send(2, 0, 4, 6).start()
        self.send(2, 0, 1, 7).start()
        self.wait_in(4, 1)
        self.send(4, 1, 2, 8).start()
        self.send(4, 1, 1, 9).start()

    def fwd2(self):
        self.wait_in(2, 1)
        self.send(2, 1, 1, 10).start()
        self.wait_in(4, 0)
        self.send(4, 0, 1, 11).start()

    def fwd3(self):
        self.wait_in(6, 0)
        self.send(6, 0, 1, 12).start()
        self.wait_in(6, 1)
        self.send(6, 1, 1, 13).start()

    def finish(self):
        for rel in (1, 3, 5, 7):
            for h in (0, 1):
                self.wait_in(rel, h)
        for idx in range(14):
            self.send(0, 0, 1, idx).wait_send()


class _TableGather:
    def __init__(self, r, p, buf, tab, ssem, rsem):
        self.r, self.p, self.buf, self.tab, self.ssem, self.rsem = r, p, buf, tab, ssem, rsem

    def rows(self, k):
        return pl.ds(pl.multiple_of(16 * (k + self.p * (3 - 2 * k)), 16), 16)

    def own(self):
        for n, (to, k) in enumerate(((2, 0), (4, 2), (2, 1), (4, 3))):
            _rcopy(self.tab.at[self.rows(k)], self.buf.at[self.r, self.rows(k)], self.ssem.at[n],
                   self.rsem.at[2 * to + k], _flip(self.r, to)).start()
        _rcopy(self.tab, self.buf.at[self.r], self.ssem.at[4], self.rsem.at[0], _flip(self.r, 1)).start()

    def wait_in(self, rel, k):
        src = self.buf.at[_flip(self.r, rel), self.rows(k)]
        _rcopy(src, src, self.ssem.at[0], self.rsem.at[2 * rel + k], _flip(self.r, 1)).wait_recv()

    def fwd(self, rel, k, to, idx):
        src = self.buf.at[_flip(self.r, rel), self.rows(k)]
        _rcopy(src, src, self.ssem.at[idx], self.rsem.at[2 * (rel ^ to) + k], _flip(self.r, to)).start()

    def twin(self, rel, k, idx):
        src = self.buf.at[_flip(self.r, rel), self.rows(k)]
        _rcopy(src, src, self.ssem.at[idx], self.rsem.at[2 * rel + 3 - k], self.r, 1 - self.p).start()

    def block(self, rel, idx, start):
        src = self.buf.at[_flip(self.r, rel)]
        c = _rcopy(src, src, self.ssem.at[idx], self.rsem.at[rel // 2], _flip(self.r, 1))
        if start:
            c.start()
        else:
            c.wait_recv()

    def relay(self, n):
        for rel, k, to in ((2, n, 4), (4, 2 + n, 2)):
            self.wait_in(rel, k)
            if n == 0:
                self.fwd(rel, k, to, 5 + rel // 4)
            self.twin(rel, k, 9 + 2 * n + (rel // 4))

    def diagonal(self):
        for n, k in enumerate((0, 2)):
            self.wait_in(6, k)
            self.twin(6, k, 7 + n)

    def blocks(self):
        for n, (rel, ks) in enumerate(((2, (2, 3)), (4, (0, 1)))):
            for k in ks:
                self.wait_in(rel, k)
            self.block(rel, 13 + n, True)

    def last_block(self):
        for k in (1, 3):
            self.wait_in(6, k)
        self.block(6, 15, True)

    def finish(self):
        _rcopy(self.tab, self.buf.at[self.r], self.ssem.at[4], self.rsem.at[0], _flip(self.r, 1)).wait_recv()
        for n, rel in enumerate((2, 4, 6)):
            self.block(rel, 13 + n, False)
        small = self.buf.at[self.r, self.rows(0)]
        for n in range(16):
            src = self.buf.at[self.r] if n in (4, 13, 14, 15) else small
            _rcopy(src, src, self.ssem.at[n], self.rsem.at[0], _flip(self.r, 1)).wait_send()


def _k1(ids, gain, tab, w, du, dres, u_out, x_out, n_out, de_out, dg_out,
        du_v, w_v, etab, dn_v, rx1, tx2, rx2, own, wc_v, u_v, n_v, nh_v, inv_v, x_v, dres_v, dx_all, dgs,
        lsem, wsem, wcsem, usem, e_s, e_r, s1, r1, s2, r2, a_s, a_r, g_s, g_r):
    r = lax.axis_index("tp")
    p = lax.axis_index("dp")
    core = lax.rem(r, 2)
    xs = lax.rem(lax.div(r, 2), 2)
    ys = lax.div(r, 4)
    cols = w.shape[1]
    n_u = cols // UC

    du_cp = pltpu.make_async_copy(du, du_v, lsem.at[0])
    du_cp.start()

    def w_cp(j, slot):
        return pltpu.make_async_copy(w.at[pl.ds(pl.multiple_of(j * FB, FB), FB)], w_v.at[slot], wsem.at[slot])

    def wc_cp(i, slot):
        return pltpu.make_async_copy(w.at[:, pl.ds(pl.multiple_of(i * UC, UC), UC)], wc_v.at[slot], wcsem.at[slot])

    def u_cp(i, slot):
        return pltpu.make_async_copy(u_v.at[slot], u_out.at[:, pl.ds(pl.multiple_of(i * UC, UC), UC)], usem.at[slot])

    for k in range(WS - 1):
        w_cp(k, k).start()
    tab_cp = pltpu.make_async_copy(tab, etab.at[r], lsem.at[2])
    tab_cp.start()
    dres_cp = pltpu.make_async_copy(dres, dres_v, lsem.at[3])
    dres_cp.start()

    barrier = pltpu.get_barrier_semaphore()
    for rel in range(1, 8):
        pl.semaphore_signal(barrier, inc=1, device_id={"tp": _flip(r, rel)}, device_id_type=MESH)
    pl.semaphore_signal(barrier, inc=1, device_id={"dp": 1 - p, "tp": r}, device_id_type=MESH)
    pl.semaphore_wait(barrier, 8)

    eg = _TableGather(r, p, etab, tab, e_s, e_r)
    eg.own()
    du_cp.wait()

    def rs1(j, m, even):
        if even:
            sib = dn_v.at[j, m, :, xs, 1 - core]
            far = [dn_v.at[j, m, :, 1 - xs, c] for c in range(2)]
            dev = [(ys * 2 + 1 - xs) * 2 + c for c in range(2)]
        else:
            sib = dn_v.at[j, m, ys, :, 1 - core]
            far = [dn_v.at[j, m, 1 - ys, :, c] for c in range(2)]
            dev = [((1 - ys) * 2 + xs) * 2 + c for c in range(2)]
        out = [_rcopy(far[c], rx1.at[j, m, 1 + core], s1.at[j, m, 1 + c], r1.at[j, m, 1 + core], dev[c])
               for c in range(2)]
        out.append(_rcopy(sib, rx1.at[j, m, 0], s1.at[j, m, 0], r1.at[j, m, 0], _flip(r, 1)))
        return out

    def rs1_start(j, m):
        if isinstance(j, int):
            for c in rs1(j, m, j % 2 == 0):
                c.start()
            return

        @pl.when(lax.rem(j, 2) == 0)
        def _():
            for c in rs1(j, m, True):
                c.start()

        @pl.when(lax.rem(j, 2) == 1)
        def _():
            for c in rs1(j, m, False):
                c.start()

    def combine(m, pair):
        for j in (2 * pair, 2 * pair + 1):
            oy, ox, q = (1 - ys, xs, ys) if j % 2 == 0 else (ys, 1 - xs, xs)
            for n in range(3):
                _rcopy(rx1.at[j, m, n], rx1.at[j, m, n], s1.at[j, m, 0], r1.at[j, m, n], _flip(r, 1)).wait_recv()

            def total(part, qi):
                t = part.astype(F32)
                for n in range(3):
                    t = t + rx1[j, m, n, qi].astype(F32)
                return t

            tx2[m, j] = total(dn_v[j, m, oy, ox, core], 1 - q)
            own[m, j] = total(dn_v[j, m, ys, xs, core], q)

    def rs2(m, j):
        oy, ox = (1 - ys, xs) if j % 2 == 0 else (ys, 1 - xs)
        return _rcopy(tx2.at[m, j], rx2.at[m, j], s2.at[m, j], r2.at[m, j], (oy * 2 + ox) * 2 + core)

    def rs2_start(m, pair):
        rs2(m, 2 * pair).start()
        rs2(m, 2 * pair + 1).start()

    def dn_step(j, carry):
        slot = lax.rem(j, WS)
        w_cp(j, slot).wait()

        @pl.when(j + WS - 1 < NB)
        def _():
            w_cp(j + WS - 1, lax.rem(j + WS - 1, WS)).start()

        part = lax.dot_general(du_v[...], w_v[slot], (((1,), (1,)), ((), ())),
                               preferred_element_type=F32)
        dn_v[j] = part.astype(BF16).reshape(2, 2, 2, 2, 32, FB)

        for n in range(2):
            @pl.when(j == n)
            def _():
                eg.relay(n)

        @pl.when(j > 0)
        def _():
            rs1_start(j - 1, 0)

        @pl.when(j > 3)
        def _():
            rs1_start(j - 4, 1)

        @pl.when(j == 3)
        def _():
            eg.diagonal()

        @pl.when(j == 7)
        def _():
            eg.blocks()

        @pl.when(j == 6)
        def _():
            combine(0, 0)

        @pl.when(j == 7)
        def _():
            rs2_start(0, 0)
            combine(0, 1)

        @pl.when(j == NB - 2)
        def _():
            for k in range(CS - 1):
                wc_cp(k, k).start()

        return carry

    lax.fori_loop(0, NB, dn_step, 0)
    tab_cp.wait()
    rs1_start(7, 0)
    rs2_start(0, 1)
    rs1_start(4, 1)
    rs1_start(5, 1)
    eg.last_block()
    eg.finish()

    gf = gain[...].astype(F32).reshape(1, 4096)

    def one_hot(first, rows, tok):
        return (tok == first + lax.broadcasted_iota(jnp.int32, (rows, tok.shape[1]), 0)).astype(BF16)

    def lookup(pick_t):
        return lax.dot_general(pick_t, etab[...].reshape(512, 4096), (((0,), (0,)), ((), ())),
                               preferred_element_type=F32)

    for b in range(512 // TB):
        rows = slice(b * TB, (b + 1) * TB)
        col = b * TB % 256
        xg = lookup(one_hot(0, 512, ids[b * TB // 256:b * TB // 256 + 1, col:col + TB]))
        inv = lax.rsqrt(jnp.mean(xg * xg, axis=-1, keepdims=True) + NORM_EPS)
        n_v[rows, :] = (xg * inv * gf).astype(BF16)

    n_cp = pltpu.make_async_copy(n_v, n_out, lsem.at[0])
    n_cp.start()

    mine = (lax.broadcasted_iota(jnp.int32, (32, 256), 1) ==
            r * 32 + lax.broadcasted_iota(jnp.int32, (32, 256), 0)).astype(BF16)
    pick_own = jnp.concatenate(
        [lax.dot_general(mine, one_hot(0, 512, ids[m:m + 1, :]), (((1,), (1,)), ((), ())), preferred_element_type=F32)
         for m in range(2)], axis=0).astype(BF16)
    xo = jnp.dot(pick_own, etab[...].reshape(512, 4096), preferred_element_type=F32)
    inv_own = lax.rsqrt(jnp.mean(xo * xo, axis=-1, keepdims=True) + NORM_EPS)
    x_v[...] = xo.astype(BF16).reshape(2, 32, 4096)
    nh_v[...] = xo * inv_own
    inv_v[...] = jnp.broadcast_to(inv_own, (64, 128))
    x_cp = pltpu.make_async_copy(x_v, x_out, lsem.at[1])
    x_cp.start()

    def dx_of(m):
        rows = slice(32 * m, 32 * m + 32)
        centre = jnp.zeros((32, 1), F32)
        for j in range(NB):
            sl = slice(j * FB, (j + 1) * FB)
            rs2(m, j).wait_recv()
            dn = own[m, j] + rx2[m, j]
            own[m, j] = dn
            nh = nh_v[rows, sl]
            centre = centre + jnp.sum(nh * (gf[:, sl] * dn), axis=-1, keepdims=True)
            part = jnp.sum(dn * nh, axis=0, keepdims=True)
            dgs[r, :, sl] = part if m == 0 else dgs[r, :, sl] + part
        centre = centre * (1.0 / 4096)
        for j in range(NB):
            sl = slice(j * FB, (j + 1) * FB)
            dr = dres_v[m, :, sl].astype(F32)
            dx = dr + inv_v[rows, 0:1] * (gf[:, sl] * own[m, j] - nh_v[rows, sl] * centre)
            dx_all[m, r, :, sl] = dx.astype(BF16)

    def dx_gather(m):
        return _Gather(r, lambda owner, h: dx_all.at[m, owner, pl.ds(16 * h, 16)], a_s.at[m], a_r.at[m])

    ag = [dx_gather(m) for m in range(2)]
    dres_cp.wait()
    events = {
        0: lambda: (combine(0, 2),),
        1: lambda: (rs2_start(0, 2), combine(0, 3),),
        2: lambda: (rs2_start(0, 3), rs1_start(6, 1), rs1_start(7, 1), combine(1, 0),),
        3: lambda: (rs2_start(1, 0), combine(1, 1),),
        4: lambda: (rs2_start(1, 1), combine(1, 2),),
        5: lambda: (rs2_start(1, 2), dx_of(0),),
        6: lambda: (combine(1, 3),),
        7: lambda: (rs2_start(1, 3), ag[0].own(),),
        9: lambda: (dx_of(1),),
        10: lambda: (ag[1].own(),),
        11: lambda: (ag[0].fwd1(),),
        13: lambda: (ag[0].fwd2(),),
        15: lambda: (ag[1].fwd1(),),
    }

    def u_step(i, carry):
        slot = lax.rem(i, 2)
        wslot = lax.rem(i, CS)
        wc_cp(i, wslot).wait()

        @pl.when(i + CS - 1 < n_u)
        def _():
            wc_cp(i + CS - 1, lax.rem(i + CS - 1, CS)).start()

        @pl.when(i >= 2)
        def _():
            u_cp(i - 2, slot).wait()

        u_v[slot] = jnp.dot(n_v[...], wc_v[wslot], preferred_element_type=F32).astype(BF16)
        u_cp(i, slot).start()

        for at, event in events.items():
            pl.when(i == at)(lambda event=event: (event(), None)[1])

        return carry

    lax.fori_loop(0, n_u, u_step, 0)
    def dg_cp(rel):
        return _rcopy(dgs.at[r], dgs.at[r], g_s.at[rel], g_r.at[r], _flip(r, rel))

    for rel in range(1, 8):
        dg_cp(rel).start()
    ag[0].fwd3()
    u_cp(n_u - 2, n_u % 2).wait()
    u_cp(n_u - 1, (n_u - 1) % 2).wait()
    ag[0].finish()
    ag[1].fwd2()

    def grad_rows(m):
        return jnp.dot(one_hot(r * 64, 64, ids[m:m + 1, :]), dx_all[m].reshape(256, 4096), preferred_element_type=F32)

    de = grad_rows(0)
    ag[1].fwd3()
    for rel in range(1, 8):
        src = _flip(r, rel)
        _rcopy(dgs.at[src], dgs.at[src], g_s.at[rel], g_r.at[src], src).wait_recv()
    tot = dgs[0]
    for k in range(1, 8):
        tot = tot + dgs[k]
    dg_out[...] = tot
    ag[1].finish()
    de_out[...] = de + grad_rows(1)

    for rel in range(1, 8):
        dg_cp(rel).wait_send()
    for m in range(2):
        for j in range(NB):
            for c in rs1(j, m, j % 2 == 0):
                c.wait_send()
            rs2(m, j).wait_send()
    n_cp.wait()
    x_cp.wait()


def _k2(n_in, du_in, u_in, x_in, de_in, dg_in, dw_out, u_out, x_out, de_out, dg_out,
        n_v, du_v, ring, u_v, x_v, de_v, dg_v, lsem, psem, qsem, osem):
    steps = n_in.shape[1] // DF
    half = 9 * 256
    cols = du_in.shape[1]
    parts = (pl.ds(0, half), pl.ds(half, cols - half))
    cp = pltpu.make_async_copy
    loads = [cp(n_in.at[:, pl.ds(0, DF)], n_v.at[:, pl.ds(0, DF)], lsem.at[0]),
             cp(du_in.at[:, parts[0]], du_v.at[:, parts[0]], lsem.at[1]),
             cp(du_in.at[:, parts[1]], du_v.at[:, parts[1]], lsem.at[2]),
             cp(n_in.at[:, pl.ds(DF, (steps - 1) * DF)], n_v.at[:, pl.ds(DF, (steps - 1) * DF)], lsem.at[3])]
    through = ((u_in, u_v, u_out), (x_in, x_v, x_out), (de_in, de_v, de_out), (dg_in, dg_v, dg_out))
    ins = [cp(a, b, psem.at[k]) for k, (a, b, _) in enumerate(through)]
    outs = [cp(b, c, qsem.at[k]) for k, (_, b, c) in enumerate(through)]
    for c in loads + ins:
        c.start()

    def store(i, slot):
        return cp(ring.at[slot], dw_out.at[pl.ds(pl.multiple_of(i * DF, DF), DF)], osem.at[slot])

    loads[0].wait()
    loads[1].wait()

    def step(i, carry):
        slot = lax.rem(i, RS)
        sl = pl.ds(pl.multiple_of(i * DF, DF), DF)

        @pl.when(i >= RS)
        def _():
            store(i - RS, slot).wait()

        @pl.when(i == 1)
        def _():
            loads[3].wait()

        @pl.when(i == 0)
        def _():
            loads[2].wait()

        ring[slot] = lax.dot_general(n_v[:, sl], du_v[...], (((0,), (0,)), ((), ())), preferred_element_type=F32)
        store(i, slot).start()

        @pl.when(i == 2)
        def _():
            for a, b in zip(ins, outs):
                a.wait()
                b.start()

        return carry

    lax.fori_loop(0, steps, step, 0)
    for i in range(steps - RS, steps):
        store(i, i % RS).wait()
    for c in outs:
        c.wait()


def solution(mesh):
    group_size = mesh.shape['tp']

    def local_step(token_ids, table_loc, gain_vec, w_loc, du_loc, dres_loc):
        num_micro, seq_len = token_ids.shape
        rows_loc, model_dim = table_loc.shape
        seq_loc = seq_len // group_size
        cols_loc = w_loc.shape[1]
        tokens = num_micro * seq_len
        du_flat = du_loc.reshape(tokens, cols_loc)
        vm, hb = pl.BlockSpec(memory_space=pltpu.VMEM), pl.BlockSpec(memory_space=pl.ANY)
        sd = jax.ShapeDtypeStruct
        dma = pltpu.SemaphoreType.DMA
        u_all, x_own, normed, grad_table, grad_gain = pl.pallas_call(
            _k1,
            out_shape=(sd((tokens, cols_loc), BF16), sd((num_micro, seq_loc, model_dim), BF16),
                       sd((tokens, model_dim), BF16), sd((rows_loc, model_dim), F32), sd((1, model_dim), F32)),
            in_specs=[vm, vm, hb, hb, hb, hb],
            out_specs=(hb, hb, hb, vm, vm),
            scratch_shapes=[
                pltpu.VMEM((tokens, cols_loc), BF16),
                pltpu.VMEM((WS, FB, cols_loc), BF16),
                pltpu.VMEM((8, 64, model_dim), BF16),
                pltpu.VMEM((NB, 2, 2, 2, 2, 32, FB), BF16),
                pltpu.VMEM((NB, 2, 3, 2, 32, FB), BF16),
                pltpu.VMEM((2, NB, 32, FB), F32),
                pltpu.VMEM((2, NB, 32, FB), F32),
                pltpu.VMEM((2, NB, 32, FB), F32),
                pltpu.VMEM((CS, model_dim, UC), BF16),
                pltpu.VMEM((2, tokens, UC), BF16),
                pltpu.VMEM((tokens, model_dim), BF16),
                pltpu.VMEM((64, model_dim), F32),
                pltpu.VMEM((64, 128), F32),
                pltpu.VMEM((2, 32, model_dim), BF16),
                pltpu.VMEM((2, 32, model_dim), BF16),
                pltpu.VMEM((2, 8, 32, model_dim), BF16),
                pltpu.VMEM((8, 1, model_dim), F32),
                dma((4,)), dma((WS,)), dma((CS,)), dma((2,)),
                dma((16,)), dma((16,)),
                dma((NB, 2, 3)), dma((NB, 2, 3)), dma((2, NB)), dma((2, NB)),
                dma((2, 14)), dma((2, 16)),
                dma((8,)), dma((8,)),
            ],
            compiler_params=pltpu.CompilerParams(collective_id=0, has_side_effects=True,
                                                 vmem_limit_bytes=67043328),
            name="k1",
        )(token_ids, gain_vec, table_loc, w_loc,
          du_flat, dres_loc)
        grad_w, u_all, x_own, grad_table, grad_gain = pl.pallas_call(
            _k2,
            out_shape=(sd((model_dim, cols_loc), F32), sd((tokens, cols_loc), BF16),
                       sd((num_micro, seq_loc, model_dim), BF16), sd((rows_loc, model_dim), F32),
                       sd((1, model_dim), F32)),
            in_specs=[hb] * 6,
            out_specs=(hb,) * 5,
            scratch_shapes=[
                pltpu.VMEM((tokens, model_dim), BF16), pltpu.VMEM((tokens, cols_loc), BF16),
                pltpu.VMEM((RS, DF, cols_loc), F32),
                pltpu.VMEM((tokens, cols_loc), BF16), pltpu.VMEM((num_micro, seq_loc, model_dim), BF16),
                pltpu.VMEM((rows_loc, model_dim), F32), pltpu.VMEM((1, model_dim), F32),
                dma((4,)), dma((4,)), dma((4,)), dma((RS,)),
            ],
            compiler_params=pltpu.CompilerParams(vmem_limit_bytes=60 * 2 ** 20),
            name="k2",
        )(normed, du_flat, u_all, x_own, grad_table, grad_gain)
        return u_all.reshape(num_micro, seq_len, cols_loc), x_own, grad_table, grad_w, grad_gain.reshape(model_dim)

    return jax.shard_map(local_step, mesh=mesh,
                         in_specs=(P('dp', None), P('tp', None), P(None), P(None, 'tp'), P('dp', None, 'tp'), P('dp', 'tp', None)),
                         out_specs=(P('dp', None, 'tp'), P('dp', 'tp', None), P(('dp', 'tp'), None), P(None, ('dp', 'tp')), P('dp')),
                         check_vma=False)
```
